128 devices in a mesh: section: 4 (over z), shard: 32 (over y, x, core).
Axes of the slice: x: 4, y: 4, z: 4, core: 2. Of those that a mesh axis runs over, the one named last changes fastest.
Arguments:
- grad_parts: bfloat16 [4, 32, 1024, 8192], P('section', 'shard'), may hold values from -6 to 6
- params: bfloat16 [4, 1024, 8192], P('section', 'shard'), may hold values from -6 to 6
- moment_first: float32 [4, 1024, 8192], P('section', 'shard'), may hold values from -6 to 6
- moment_second: float32 [4, 1024, 8192], P('section', 'shard'), may hold values from 0.5 to 50
- block_layer: int32 [4, 128], P('section', 'shard'), may hold values from 0 to 7, as said below
- block_valid: int32 [4, 128], P('section', 'shard'), may hold values from 0 to 1
- decay: float32 [8], replicated, may hold values from 0.05 to 1
Outputs:
- new_params: bfloat16 [4, 1024, 8192], P('section', 'shard')
- new_first: float32 [4, 1024, 8192], P('section', 'shard')
- new_second: float32 [4, 1024, 8192], P('section', 'shard')
- ratios: float32 [8], replicated
The draws below stay inside these ranges and needn't reach their ends.
Inputs may be any that keep to these rules, and one draw needn't show every extreme that they name: `block_layer`: in every section the live slots come first. One section has all 128 slots live; each other section has between 64 and 128 live slots, and all sections together have 3 * 128. Over the live slots taken section by section in order, layer ids never fall and every layer has exactly 48 live slots; dead slots hold arbitrary layer ids.
All inputs are finite; a program needn't handle non-finite values.
Results may differ from the reference program's by a relative error of at most 0.008.
Values may be sent and summed in bfloat16 or wider, within the bound.
A program may use at most 64 MiB of HBM per device.

```python
import math
import jax
import jax.numpy as jnp
from jax import lax

D = 8192
LAYERS = 8
BLOCK = 8
SECTION_BLK = 128
SECTION_ROWS = 1024
LAYER_BLK = 48
N_SECTION = 4
N_SHARD = 32


def layout(key):
    keyed = jax.random.fold_in(key, 11)
    full = SECTION_BLK
    half_blk = SECTION_BLK // 2
    first_count = jax.random.randint(jax.random.fold_in(keyed, 3), (), half_blk, full + 1)
    lower = jnp.maximum(half_blk, full - first_count)
    upper = jnp.minimum(full, 3 * half_blk - first_count)
    second_count = jax.random.randint(jax.random.fold_in(keyed, 4), (), lower, upper + 1)
    third_count = 2 * full - first_count - second_count
    base = jnp.stack([jnp.array(full, jnp.int32), first_count.astype(jnp.int32), second_count.astype(jnp.int32), third_count.astype(jnp.int32)])
    order = jax.random.permutation(jax.random.fold_in(keyed, 1), 4)
    counts = base[order]
    offsets = jnp.cumsum(counts) - counts
    slots = jnp.arange(SECTION_BLK, dtype=jnp.int32)
    valid = slots[None, :] < counts[:, None]
    position = offsets[:, None] + slots[None, :]
    layer = position // LAYER_BLK
    filler = jax.random.randint(jax.random.fold_in(keyed, 2), (4, SECTION_BLK), 0, LAYERS)
    return (jnp.where(valid, layer, filler).astype(jnp.int32), valid.astype(jnp.int32))


def draw_block_layer(key, part):
    return layout(key)[0]


def draw_block_valid(key, part):
    return layout(key)[1]


def strengthened(result, key, source, target, blocks, factor):
    owner, partner = [(jnp.arange(result.shape[dim]) // (result.shape[dim] // blocks)).reshape([-1 if axis == dim else 1 for axis in range(result.ndim)]) for dim in (source, target)]
    chosen = jax.random.permutation(key, blocks)[partner]
    strong = (owner == chosen) | (owner == (partner + blocks // 2) % blocks)
    return jnp.where(strong, factor * result, result)


def level_of(own_key, shape, shards, least, top_value):
    factor_of, own = 1.0, jax.random.fold_in(own_key, 6)
    for axis_at, blocks in shards:
        heights = jnp.exp(jax.random.uniform(jax.random.fold_in(own, axis_at), (blocks,), jnp.float32, least / len(shards), top_value / len(shards)))
        factor_of = factor_of * jnp.repeat(heights, shape[axis_at] // blocks).reshape([-1 if axis == axis_at else 1 for axis in range(len(shape))])
    return factor_of


def centred(stream_key, shape, spread, bound, split=(), kind=jnp.bfloat16):
    loudness = level_of(stream_key, shape, split, -0.22, 0.18) if split else 1.0
    result = jax.random.normal(stream_key, shape, jnp.float32) * spread * loudness
    return jnp.minimum(jnp.maximum(result, -bound), bound).astype(kind)


def noise_with(key, dims, width, bound, pieces, heavy, kind=jnp.bfloat16):
    entries = width * jax.random.normal(key, dims, jnp.float32)
    if pieces:
        entries = entries * level_of(key, dims, pieces, -0.22, 0.18)
    return jnp.clip(strengthened(entries, jax.random.fold_in(key, 3), *heavy), -bound, bound).astype(kind)


def setup_inputs(seed: int = 0) -> dict:
    seeds = jax.random.split(jax.random.key(seed), 8)
    return {
        "grad_parts": noise_with(seeds[0], (N_SECTION, N_SHARD, SECTION_ROWS, D), 1.0, 6.0, ((0, 4), (1, 32)), (1, 2, 32, 2.75)),
        "params": centred(seeds[1], (N_SECTION, SECTION_ROWS, D), 1.0, 6.0, ((0, 4), (1, 32))),
        "moment_first": centred(seeds[2], (N_SECTION, SECTION_ROWS, D), 1.0, 6.0, ((0, 4), (1, 32)), jnp.float32),
        "moment_second": jnp.clip(jnp.exp(math.log(50.0) - 4.6051702 * jax.random.uniform(seeds[3], (N_SECTION, SECTION_ROWS, D), jnp.float32) ** level_of(seeds[3], (N_SECTION, SECTION_ROWS, D), ((0, 4), (1, 32)), -0.2, 0.2)), 0.5, 50.0),
        "block_layer": draw_block_layer(jax.random.fold_in(seeds[7], 71), 0),
        "block_valid": draw_block_valid(jax.random.fold_in(seeds[7], 71), 0),
        "decay": jnp.clip(jnp.exp(jax.random.uniform(seeds[6], (LAYERS,), jnp.float32, math.log(0.05), math.log(1.0))), 0.05, 1.0),
    }


bias_first = 1.0 - 0.9 ** 10
bias_second = 1.0 - 0.99 ** 10

def reference(grad_parts, params, moment_first, moment_second, block_layer, block_valid, decay):

    def add_part(index, running):
        return running + lax.dynamic_index_in_dim(grad_parts, index, 1, keepdims=False).astype(jnp.float32)
    initial = jnp.zeros((grad_parts.shape[0], grad_parts.shape[2], grad_parts.shape[3]), jnp.float32)
    gradient = lax.fori_loop(0, grad_parts.shape[1], add_part, initial)
    first = 0.9 * moment_first + 0.1 * gradient
    second = 0.99 * moment_second + 0.01 * gradient * gradient
    layer_rows = jnp.repeat(block_layer, BLOCK, axis=1)
    valid_rows = jnp.repeat(block_valid, BLOCK, axis=1) > 0
    weights = params.astype(jnp.float32)
    update = first / bias_first / (jnp.sqrt(second / bias_second) + 1e-06) + decay[layer_rows][..., None] * weights
    onehot = jnp.where(valid_rows[..., None] & (layer_rows[..., None] == jnp.arange(LAYERS, dtype=jnp.int32)), 1.0, 0.0).astype(jnp.float32)
    weight_sq = lax.optimization_barrier(jnp.sum(weights * weights, axis=-1))
    update_sq = lax.optimization_barrier(jnp.sum(update * update, axis=-1))
    wsum = jnp.einsum('sr,srl->l', weight_sq, onehot, precision=lax.Precision.HIGHEST)
    usum = jnp.einsum('sr,srl->l', update_sq, onehot, precision=lax.Precision.HIGHEST)
    ratios = jnp.sqrt(wsum / (usum + 1.0))
    row_ratio = ratios[layer_rows]
    stepped = weights - 0.1 * row_ratio[..., None] * update
    new_params = jnp.where(valid_rows[..., None], stepped, weights).astype(jnp.bfloat16)
    new_first = jnp.where(valid_rows[..., None], first, moment_first)
    new_second = jnp.where(valid_rows[..., None], second, moment_second)
    return (new_params, new_first, new_second, ratios)
```

```python
import functools

import jax
import jax.numpy as jnp
from jax import lax
from jax.experimental import pallas as pl
from jax.experimental.pallas import tpu as pltpu
from jax.sharding import PartitionSpec as P

bias_first = 1.0 - 0.9**10
bias_second = 1.0 - 0.99**10

MESH = pl.DeviceIdType.MESH
F32, BF16 = jnp.float32, jnp.bfloat16
SIDE = 4
ORDER = (2, 1, 3, 0)
FAR, NEAR_OWN, NEAR_SUM = (0, 1, 2, 3), (4, 6, 8, 10), (5, 7, 9, 11)
FAR2, OWN2, SUM2 = 12, 13, 14
SLOTS = 15


def block_at(axis, main, other):
    return other * SIDE + main if axis == 0 else main * SIDE + other


def kernel(
    n_section, n_shard,
    grads, params, m_first, m_second, layer, valid, decay,
    out_params, out_first, out_second, out_ratios,
    mine, theirs, landed, w_buf, f_buf, s_buf, upd, sums, got,
    load_sem, pair_send, pair_recv, link_send, link_recv, io_sem, out_sem, sum_send, sum_recv,
):
    rows = w_buf.shape[0]
    width = landed.shape[3]
    section, shard = lax.axis_index("section"), lax.axis_index("shard")
    core, x, y = shard % 2, (shard // 2) % SIDE, shard // (2 * SIDE)
    me = section * n_shard + shard
    partner = shard + 1 - 2 * core

    def shard_at(dy, dx):
        return (((y + dy) % SIDE) * SIDE + (x + dx) % SIDE) * 2 + core

    links = (shard_at(0, 1), shard_at(0, 3), shard_at(1, 0), shard_at(3, 0))

    barrier = pltpu.get_barrier_semaphore()
    for peer in (partner,) + links:
        pl.semaphore_signal(barrier, inc=1, device_id={"shard": peer}, device_id_type=MESH)
    for k in range(1, n_section):
        pl.semaphore_signal(
            barrier, inc=1, device_id={"section": (section + k) % n_section}, device_id_type=MESH
        )

    order = []
    for j in ORDER:
        order += [(h, block_at(h, 2, j)) for h in (0, 1)]
    for j in ORDER:
        for main in (1, 3, 0):
            order += [(h, block_at(h, main, j)) for h in (0, 1)]

    def rows_of(block, which):
        dy, dx = block // SIDE, block % SIDE
        chip = ((y + dy) % SIDE) * SIDE + (x + dx) % SIDE
        return pl.ds(pl.multiple_of(chip * (2 * rows) + which * rows, rows), rows)

    def load(h, block):
        return pltpu.make_async_copy(
            grads.at[0, 0, rows_of(block, core), pl.ds(h * 2 * width, 2 * width)],
            mine.at[h, block],
            load_sem.at[h, block],
        )

    def pair(h, block):
        return pltpu.make_async_remote_copy(
            src_ref=grads.at[0, 0, rows_of(block, 1 - core), pl.ds(h * 2 * width, 2 * width)],
            dst_ref=theirs.at[h, block],
            send_sem=pair_send.at[h, block],
            recv_sem=pair_recv.at[h, block],
            device_id={"shard": partner},
            device_id_type=MESH,
        )

    def quarter(ref, h, block, q):
        return ref.at[h, block, :, pl.ds(q * width, width)]

    def send(link, slot, src):
        return pltpu.make_async_remote_copy(
            src_ref=src,
            dst_ref=landed.at[link, slot],
            send_sem=link_send.at[link, slot],
            recv_sem=link_recv.at[link, slot],
            device_id={"shard": links[link]},
            device_id_type=MESH,
        )

    def arrived(link, slot):
        send(link, slot, landed.at[link, slot]).wait_recv()
        return landed.at[link, slot]

    def add_up(dst, terms):
        step = min(512, width)

        def one(i, _):
            cols = pl.ds(pl.multiple_of(i * step, step), step)
            total = terms[0][:, cols].astype(F32)
            for t in terms[1:]:
                total = total + t[:, cols].astype(F32)
            dst[:, cols] = total.astype(BF16)
            return 0

        lax.fori_loop(0, width // step, one, 0)

    for h, block in order:
        load(h, block).start()
    pl.semaphore_wait(barrier, 1 + len(links) + n_section - 1)
    for h, block in order:
        pair(h, block).start()
    io = [
        pltpu.make_async_copy(params.at[0], w_buf, io_sem.at[0]),
        pltpu.make_async_copy(m_first.at[0], f_buf, io_sem.at[1]),
        pltpu.make_async_copy(m_second.at[0], s_buf, io_sem.at[2]),
    ]
    for c in io:
        c.start()

    ready = set()

    def need(h, block):
        if (h, block) not in ready:
            ready.add((h, block))
            load(h, block).wait()
            pair(h, block).wait_recv()

    def put(link, slot, h, block, q, extra=()):
        need(h, block)
        dst = quarter(mine, h, block, q)
        add_up(dst, [dst, quarter(theirs, h, block, q), *extra])
        send(link, slot, dst).start()

    signs = (1, 3)

    def far(j):
        for axis in (0, 1):
            for d in (0, 1):
                put(2 * axis + d, FAR[j], axis, block_at(axis, 2, ORDER[j]), d)

    def near_own(j):
        for axis in (0, 1):
            for d in (0, 1):
                put(2 * axis + d, NEAR_OWN[j], axis, block_at(axis, signs[d], ORDER[j]), 1 - d)

    def near_sum(j):
        for axis in (0, 1):
            for d in (0, 1):
                link = 2 * axis + d
                put(link, NEAR_SUM[j], axis, block_at(axis, signs[d], ORDER[j]), d, [arrived(link, FAR[j])])

    def first_axis(axis, j):
        block = block_at(axis, 0, ORDER[j])
        need(axis, block)
        a, b = 2 * axis, 2 * axis + 1
        came = [arrived(link, slot) for link in (a, b) for slot in (NEAR_OWN[j], NEAR_SUM[j])]
        return block, ((came[1], came[2]), (came[3], came[0]))

    def settle(j):
        for axis in (0, 1):
            block, came = first_axis(axis, j)
            for q in (0, 1):
                dst = quarter(mine, axis, block, q)
                add_up(dst, [dst, quarter(theirs, axis, block, q), *came[q]])

    def far2():
        settle(0)
        for axis in (0, 1):
            for d in (0, 1):
                link = 2 * (1 - axis) + d
                send(link, FAR2, quarter(mine, axis, block_at(axis, 0, 2), d)).start()

    def own2():
        settle(1)
        settle(2)
        for axis in (0, 1):
            for d in (0, 1):
                link = 2 * (1 - axis) + d
                send(link, OWN2, quarter(mine, axis, block_at(axis, 0, signs[d]), 1 - d)).start()

    def sum2():
        for axis in (0, 1):
            for d in (0, 1):
                link = 2 * (1 - axis) + d
                dst = quarter(mine, axis, block_at(axis, 0, signs[d]), d)
                add_up(dst, [dst, arrived(link, FAR2)])
                send(link, SUM2, dst).start()

    for j in range(4):
        far(j)
    for j in range(3):
        near_own(j)
        near_sum(j)
    near_own(3)

    row_block = lax.broadcasted_iota(jnp.int32, (rows, 128), 0) // 8
    lane = lax.broadcasted_iota(jnp.int32, (1, 128), 1)
    blocks = rows // 8

    def per_row(values):
        out = jnp.full((rows, 128), values[0])
        for b in range(1, blocks):
            out = jnp.where(row_block == b, values[b], out)
        return out

    layers = [layer[0, b] for b in range(blocks)]
    lives = [valid[0, b] for b in range(blocks)]
    row_decay = per_row([decay[l] for l in layers])
    row_live = per_row(lives) > 0

    def by_layer(total, offset):
        out = jnp.zeros((1, 128), F32)
        for b in range(blocks):
            s = jnp.sum(total[8 * b : 8 * b + 8, :], keepdims=True)
            out = out + jnp.where((lane == layers[b] + offset) & (lives[b] > 0), s, 0.0)
        return out

    far2()
    near_sum(3)
    own2()
    sum2()

    for c in io:
        c.wait()
    columns = w_buf.shape[1]
    piece = 512

    def weights_sq(i, acc):
        for k in range(piece // 128):
            v = w_buf[:, pl.ds(pl.multiple_of(i * piece + k * 128, 128), 128)].astype(F32)
            acc = acc + v * v
        return acc

    w_sum = by_layer(lax.fori_loop(0, columns // piece, weights_sq, jnp.zeros((rows, 128), F32)), 8)

    acc = jnp.zeros((rows, 128), F32)
    for axis in (0, 1):
        block, came = first_axis(axis, 3)
        for q in (0, 1):
            a = 2 * (1 - axis)
            late = [arrived(a + q, SUM2), arrived(a + 1 - q, OWN2)]
            terms = [quarter(mine, axis, block, q), quarter(theirs, axis, block, q), *came[q], *late]
            base = (2 * axis + q) * width

            def one(i, acc, terms=terms, base=base):
                for k in range(min(512, width) // 128):
                    at = i * min(512, width) + k * 128
                    here = pl.ds(pl.multiple_of(at, 128), 128)
                    cols = pl.ds(pl.multiple_of(base + at, 128), 128)
                    g = terms[0][:, here].astype(F32)
                    for t in terms[1:]:
                        g = g + t[:, here].astype(F32)
                    old_f, old_s = f_buf[:, cols], s_buf[:, cols]
                    w = w_buf[:, cols].astype(F32)
                    first = 0.9 * old_f + 0.1 * g
                    second = 0.99 * old_s + 0.01 * g * g
                    u = (first * (1.0 / bias_first)) / (
                        jnp.sqrt(second * (1.0 / bias_second)) + 1e-06
                    ) + row_decay * w
                    upd[:, cols] = u
                    f_buf[:, cols] = jnp.where(row_live, first, old_f)
                    s_buf[:, cols] = jnp.where(row_live, second, old_s)
                    acc = acc + u * u
                return acc

            acc = lax.fori_loop(0, width // min(512, width), one, acc)

    vec = by_layer(acc, 0) + w_sum
    sums[0] = vec
    got[me] = vec

    n_all = n_section * n_shard

    def to_device(k):
        other = (me + k) % n_all
        return pltpu.make_async_remote_copy(
            src_ref=sums.at[0],
            dst_ref=got.at[me],
            send_sem=sum_send,
            recv_sem=sum_recv,
            device_id={"section": other // n_shard, "shard": other % n_shard},
            device_id_type=MESH,
        )

    def tell(k, _):
        to_device(k).start()
        return 0

    lax.fori_loop(1, n_all, tell, 0)
    outs = [
        pltpu.make_async_copy(f_buf, out_first.at[0], out_sem.at[0]),
        pltpu.make_async_copy(s_buf, out_second.at[0], out_sem.at[1]),
    ]
    for c in outs:
        c.start()
    everyone = pltpu.make_async_copy(got.at[pl.ds(0, n_all - 1)], got.at[pl.ds(0, n_all - 1)], sum_recv)
    everyone.wait()

    def add_device(k, t):
        return t + got[k]

    total = lax.fori_loop(0, n_all, add_device, jnp.zeros((1, 128), F32), unroll=8)
    wide = jnp.broadcast_to(total, (8, 128))
    ratios = jnp.sqrt(pltpu.roll(wide, 120, 1) / (wide + 1.0))[0:1]
    ratios = jnp.where(lane < 8, ratios, 0.0)
    out_ratios[...] = ratios
    scale = []
    for b in range(blocks):
        r = jnp.sum(jnp.where(lane == layers[b], ratios, 0.0), keepdims=True)
        scale.append(jnp.where(lives[b] > 0, 0.1 * r, 0.0))
    row_scale = per_row(scale)

    def last(i, _):
        for k in range(piece // 128):
            cols = pl.ds(pl.multiple_of(i * piece + k * 128, 128), 128)
            w = w_buf[:, cols].astype(F32)
            w_buf[:, cols] = (w - row_scale * upd[:, cols]).astype(BF16)
        return 0

    lax.fori_loop(0, columns // piece, last, 0)
    final = pltpu.make_async_copy(w_buf, out_params.at[0], out_sem.at[2])
    final.start()

    for h, block in order:
        pair(h, block).wait_send()
    for link in range(4):
        for slot in range(SLOTS):
            send(link, slot, landed.at[link, slot]).wait_send()
    pltpu.make_async_copy(got.at[pl.ds(0, n_all - 1)], got.at[pl.ds(0, n_all - 1)], sum_send).wait()
    for c in outs:
        c.wait()
    final.wait()


def shards(grad_parts, params, moment_first, moment_second, block_layer, block_valid, decay):
    rows, columns = params.shape[1:]
    n_section, n_shard = lax.axis_size("section"), lax.axis_size("shard")
    width = columns // 4
    chips = SIDE * SIDE
    anywhere, smem = pl.BlockSpec(memory_space=pl.ANY), pl.BlockSpec(memory_space=pltpu.SMEM)
    dma = pltpu.SemaphoreType.DMA
    new_params, new_first, new_second, ratios = pl.pallas_call(
        functools.partial(kernel, n_section, n_shard),
        out_shape=(
            jax.ShapeDtypeStruct(params.shape, params.dtype),
            jax.ShapeDtypeStruct(moment_first.shape, F32),
            jax.ShapeDtypeStruct(moment_second.shape, F32),
            jax.ShapeDtypeStruct((1, 128), F32),
        ),
        in_specs=[anywhere] * 4 + [smem] * 3,
        out_specs=(anywhere, anywhere, anywhere, pl.BlockSpec(memory_space=pltpu.VMEM)),
        scratch_shapes=[
            pltpu.VMEM((2, chips, rows, 2 * width), BF16),
            pltpu.VMEM((2, chips, rows, 2 * width), BF16),
            pltpu.VMEM((4, SLOTS, rows, width), BF16),
            pltpu.VMEM((rows, columns), BF16),
            pltpu.VMEM((rows, columns), F32),
            pltpu.VMEM((rows, columns), F32),
            pltpu.VMEM((rows, columns), F32),
            pltpu.VMEM((1, 1, 128), F32),
            pltpu.VMEM((n_section * n_shard, 1, 128), F32),
            dma((2, chips)),
            dma((2, chips)),
            dma((2, chips)),
            dma((4, SLOTS)),
            dma((4, SLOTS)),
            dma((3,)),
            dma((3,)),
            dma,
            dma,
        ],
        compiler_params=pltpu.CompilerParams(
            collective_id=0, has_side_effects=True, vmem_limit_bytes=56 * 2**20
        ),
        name="lamb_step",
    )(grad_parts, params, moment_first, moment_second, block_layer, block_valid, decay)
    return new_params, new_first, new_second, ratios[0, : decay.shape[0]]


def solution(mesh):
    placed = (
        P("section", "shard", None, None),
        P("section", "shard", None),
        P("section", "shard", None),
        P("section", "shard", None),
        P("section", "shard"),
        P("section", "shard"),
        P(),
    )
    return jax.shard_map(
        shards,
        mesh=mesh,
        in_specs=placed,
        out_specs=(
            P("section", "shard", None),
            P("section", "shard", None),
            P("section", "shard", None),
            P(),
        ),
        check_vma=False,
    )
```

```python
import functools

import jax
import jax.numpy as jnp
from jax import lax
from jax.experimental import pallas as pl
from jax.experimental.pallas import tpu as pltpu
from jax.sharding import PartitionSpec as P

bias_first = 1.0 - 0.9**10
bias_second = 1.0 - 0.99**10

MESH = pl.DeviceIdType.MESH
F32, BF16 = jnp.float32, jnp.bfloat16
SIDE = 4
ORDER = (2, 1, 3, 0)
FAR, NEAR_OWN, NEAR_SUM = (0, 1, 2, 3), (4, 6, 8, 10), (5, 7, 9, 11)
FAR2, OWN2 = 12, 13
SLOTS = 14


def block_at(axis, main, other):
    return other * SIDE + main if axis == 0 else main * SIDE + other


def kernel(
    n_section, n_shard,
    grads, params, m_first, m_second, layer_hbm, valid_hbm, decay_hbm,
    upd, f_buf, s_buf, w_buf, out_scale, out_ratios,
    mine, theirs, ahead, landed, late, layer, valid, decay, sums, got,
    load_sem, pair_send, pair_recv, link_send, far_recv, near_recv, far2_recv, own2_recv, sum2_recv, sum2_send,
    io_sem, sum_send, sum_recv,
):
    rows = w_buf.shape[1]
    columns = w_buf.shape[2]
    width = landed.shape[3]
    part = late.shape[3]
    parts = width // part
    section, shard = lax.axis_index("section"), lax.axis_index("shard")
    core, x, y = lax.rem(shard, 2), lax.rem(lax.div(shard, 2), SIDE), lax.div(shard, 2 * SIDE)
    me = section * n_shard + shard
    partner = shard + 1 - 2 * core

    def chip_at(dy, dx):
        return lax.rem(y + dy, SIDE) * SIDE + lax.rem(x + dx, SIDE)

    links = tuple(chip_at(dy, dx) * 2 + core for dy, dx in ((0, 1), (0, 3), (1, 0), (3, 0)))

    barrier = pltpu.get_barrier_semaphore()
    for peer in (partner,) + links:
        pl.semaphore_signal(barrier, inc=1, device_id={"shard": peer}, device_id_type=MESH)
    for k in range(1, n_section):
        pl.semaphore_signal(
            barrier, inc=1, device_id={"section": lax.rem(section + k, n_section)}, device_id_type=MESH
        )

    groups = [[(0, block_at(0, 2, 2))], [(1, block_at(1, 2, 2))]]
    for j in ORDER[1:]:
        groups.append([(h, block_at(h, 2, j)) for h in (0, 1)])
    for j in ORDER:
        groups.append([(h, block_at(h, main, j)) for main in (1, 3, 0) for h in (0, 1)])
    group_of = {b: g for g, blocks in enumerate(groups) for b in blocks}

    def source(h, block, which):
        chip = chip_at(block // SIDE, block % SIDE)
        at = pl.multiple_of(chip * (2 * rows) + which * rows, rows)
        return grads.at[0, 0, pl.ds(at, rows), pl.ds(h * 2 * width, 2 * width)]

    def load(h, block):
        return pltpu.make_async_copy(
            source(h, block, core), mine.at[h, block], load_sem.at[group_of[h, block]]
        )

    def fetch_ahead(h):
        return pltpu.make_async_copy(source(h, block_at(h, 2, 2), 1 - core), ahead.at[h], io_sem.at[h])

    def pair(h, block):
        first = group_of[h, block] < 2
        return pltpu.make_async_remote_copy(
            src_ref=ahead.at[h] if first else source(h, block, 1 - core),
            dst_ref=theirs.at[h, block],
            send_sem=pair_send,
            recv_sem=pair_recv.at[group_of[h, block]],
            device_id={"shard": partner},
            device_id_type=MESH,
        )

    def wait_bytes(ref, sem):
        pltpu.make_async_copy(ref, ref, sem).wait()

    def quarter(ref, h, block, q):
        return ref.at[h, block, :, pl.ds(q * width, width)]

    def send(link, src, dst, recv_sem, send_sem=link_send):
        pltpu.make_async_remote_copy(
            src_ref=src,
            dst_ref=dst,
            send_sem=send_sem,
            recv_sem=recv_sem,
            device_id={"shard": links[link]},
            device_id_type=MESH,
        ).start()

    def add_up(dst, terms):
        size = dst.shape[1]
        step = min(512, size)

        def one(i, _):
            cols = pl.ds(pl.multiple_of(i * step, step), step)
            if len(terms) == 2:
                dst[:, cols] = terms[0][:, cols] + terms[1][:, cols]
            else:
                total = terms[0][:, cols].astype(F32)
                for t in terms[1:]:
                    total = total + t[:, cols].astype(F32)
                dst[:, cols] = total.astype(BF16)
            return 0

        lax.fori_loop(0, size // step, one, 0)

    for h in (0, 1):
        fetch_ahead(h).start()
        load(h, block_at(h, 2, 2)).start()
    for h, block in groups[2]:
        load(h, block).start()
    with jax.named_scope("barrier"):
        pl.semaphore_wait(barrier, 1 + len(links) + n_section - 1)
    for h in (0, 1):
        fetch_ahead(h).wait()
        pair(h, block_at(h, 2, 2)).start()
    small = [
        pltpu.make_async_copy(a, b, io_sem.at[2 + k])
        for k, (a, b) in enumerate(((layer_hbm, layer), (valid_hbm, valid), (decay_hbm, decay)))
    ]
    io = [
        pltpu.make_async_copy(params, w_buf, io_sem.at[5]),
        pltpu.make_async_copy(m_first, f_buf, io_sem.at[6]),
        pltpu.make_async_copy(m_second, s_buf, io_sem.at[7]),
    ]
    for g in range(2, len(groups)):
        for h, block in groups[g]:
            pair(h, block).start()
        if g > 2:
            for h, block in groups[g]:
                load(h, block).start()
        if g == 5:
            for c in small + io:
                c.start()

    ready = set()

    def need(h, block):
        g = group_of[h, block]
        if g not in ready:
            ready.add(g)
            several = mine.at[0, pl.ds(0, len(groups[g]))]
            wait_bytes(several, load_sem.at[g])
            wait_bytes(several, pair_recv.at[g])

    signs = (1, 3)
    each = [(axis, d, 2 * axis + d) for axis in (0, 1) for d in (0, 1)]
    four = landed.at[0, pl.ds(0, 4)]

    def own_terms(axis, block, q):
        need(axis, block)
        return [quarter(mine, axis, block, q), quarter(theirs, axis, block, q)]

    def far(j):
        for axis, d, link in each:
            terms = own_terms(axis, block_at(axis, 2, ORDER[j]), d)
            add_up(terms[0], terms)
            send(link, terms[0], landed.at[link, FAR[j]], far_recv.at[j])

    def near_own(j):
        for axis, d, link in each:
            terms = own_terms(axis, block_at(axis, signs[d], ORDER[j]), 1 - d)
            add_up(terms[0], terms)
            send(link, terms[0], landed.at[link, NEAR_OWN[j]], near_recv.at[axis, j])

    def near_sum(j):
        wait_bytes(four, far_recv.at[j])
        for axis, d, link in each:
            terms = own_terms(axis, block_at(axis, signs[d], ORDER[j]), d)
            add_up(terms[0], terms + [landed.at[link, FAR[j]]])
            send(link, terms[0], landed.at[link, NEAR_SUM[j]], near_recv.at[axis, j])

    def first_axis(axis, j):
        block = block_at(axis, 0, ORDER[j])
        wait_bytes(four, near_recv.at[axis, j])
        a, b = 2 * axis, 2 * axis + 1
        return [
            own_terms(axis, block, q)
            + [landed.at[(a, b)[q], NEAR_SUM[j]], landed.at[(b, a)[q], NEAR_OWN[j]]]
            for q in (0, 1)
        ]

    def settle(j):
        for axis in (0, 1):
            for terms in first_axis(axis, j):
                add_up(terms[0], terms)

    def far2():
        settle(0)
        for axis, d, _ in each:
            link = 2 * (1 - axis) + d
            send(link, quarter(mine, axis, block_at(axis, 0, 2), d), landed.at[link, FAR2], far2_recv)

    def own2():
        settle(1)
        settle(2)
        for axis, d, _ in each:
            link = 2 * (1 - axis) + d
            src = quarter(mine, axis, block_at(axis, 0, signs[d]), 1 - d)
            send(link, src, landed.at[link, OWN2], own2_recv)

    def sum2():
        wait_bytes(four, far2_recv)
        for p in range(parts):
            for axis, d, _ in each:
                link = 2 * (1 - axis) + d
                at = pl.ds(p * part, part)
                dst = quarter(mine, axis, block_at(axis, 0, signs[d]), d).at[:, at]
                add_up(dst, [dst, landed.at[link, FAR2].at[:, at]])
                send(link, dst, late.at[p, link], sum2_recv.at[p], sum2_send)

    for j in range(4):
        with jax.named_scope(f"far{j}"):
            far(j)
    for j in range(3):
        with jax.named_scope(f"own{j}"):
            near_own(j)
        with jax.named_scope(f"sum{j}"):
            near_sum(j)
    near_own(3)

    for c in small + io:
        c.wait()
    row_block = lax.broadcasted_iota(jnp.int32, (rows, 128), 0) // 8
    lane = lax.broadcasted_iota(jnp.int32, (1, 128), 1)
    blocks = rows // 8

    def per_row(values):
        out = jnp.full((rows, 128), values[0])
        for b in range(1, blocks):
            out = jnp.where(row_block == b, values[b], out)
        return out

    layers = [layer[0, b] for b in range(blocks)]
    lives = [valid[0, b] for b in range(blocks)]
    row_decay = per_row([decay[l] for l in layers])
    row_live = per_row(lives) > 0

    def by_layer(total, offset):
        out = jnp.zeros((1, 128), F32)
        for b in range(blocks):
            s = jnp.sum(total[8 * b : 8 * b + 8, :], keepdims=True)
            out = out + jnp.where((lane == layers[b] + offset) & (lives[b] > 0), s, 0.0)
        return out

    piece = 512

    def weights_sq(i, acc):
        for k in range(piece // 128):
            v = w_buf[0, :, pl.ds(pl.multiple_of(i * piece + k * 128, 128), 128)].astype(F32)
            acc = acc + v * v
        return acc

    w_sum = by_layer(lax.fori_loop(0, columns // piece, weights_sq, jnp.zeros((rows, 128), F32)), 8)

    with jax.named_scope("far2"):
        far2()
    with jax.named_scope("near_sum3"):
        near_sum(3)
    with jax.named_scope("own2"):
        own2()
    with jax.named_scope("sum2"):
        sum2()

    with jax.named_scope("early"):
        for axis in (0, 1):
            both = first_axis(axis, 3)
            if axis == 0:
                wait_bytes(four, own2_recv)
            for q in (0, 1):
                terms = both[q] + [landed.at[2 * (1 - axis) + 1 - q, OWN2]]
                base = (2 * axis + q) * width

                def before(i, _, terms=terms, base=base):
                    at = pl.multiple_of(i * min(512, width), min(512, width))
                    here = pl.ds(at, min(512, width))
                    g = terms[0][:, here].astype(F32)
                    for t in terms[1:]:
                        g = g + t[:, here].astype(F32)
                    upd[0, :, pl.ds(base + at, min(512, width))] = g
                    return 0

                lax.fori_loop(0, width // min(512, width), before, 0)

    acc = jnp.zeros((rows, 128), F32)
    for p in range(parts):
        with jax.named_scope(f"late{p}"):
            wait_bytes(late.at[p], sum2_recv.at[p])
        for axis in (0, 1):
            for q in (0, 1):
                came = late.at[p, 2 * (1 - axis) + q]
                base = (2 * axis + q) * width + p * part
                step = min(512, part)

                def one(i, acc, came=came, base=base, step=step):
                    for k in range(step // 128):
                        at = i * step + k * 128
                        cols = pl.ds(pl.multiple_of(base + at, 128), 128)
                        g = upd[0, :, cols] + came[:, pl.ds(pl.multiple_of(at, 128), 128)].astype(F32)
                        old_f, old_s = f_buf[0, :, cols], s_buf[0, :, cols]
                        w = w_buf[0, :, cols].astype(F32)
                        first = 0.9 * old_f + 0.1 * g
                        second = 0.99 * old_s + 0.01 * g * g
                        u = (first * (1.0 / bias_first)) / (
                            jnp.sqrt(second * (1.0 / bias_second)) + 1e-06
                        ) + row_decay * w
                        upd[0, :, cols] = u
                        f_buf[0, :, cols] = jnp.where(row_live, first, old_f)
                        s_buf[0, :, cols] = jnp.where(row_live, second, old_s)
                        acc = acc + u * u
                    return acc

                acc = lax.fori_loop(0, part // step, one, acc)

    vec = by_layer(acc, 0) + w_sum
    sums[0] = vec
    got[me] = vec

    def tell(to_section, to_shard):
        pltpu.make_async_remote_copy(
            src_ref=sums.at[0],
            dst_ref=got.at[me],
            send_sem=sum_send,
            recv_sem=sum_recv,
            device_id={"section": to_section, "shard": to_shard},
            device_id_type=MESH,
        ).start()

    sections = [lax.rem(section + k, n_section) for k in range(n_section)]

    def tell_shard(k, _):
        to_shard = lax.rem(shard + k, n_shard)
        for to_section in sections:
            tell(to_section, to_shard)
        return 0

    with jax.named_scope("tell"):
        lax.fori_loop(1, n_shard, tell_shard, 0)
        for to_section in sections[1:]:
            tell(to_section, shard)
    n_all = n_section * n_shard
    others = got.at[pl.ds(0, n_all - 1)]
    with jax.named_scope("everyone"):
        wait_bytes(others, sum_recv)

    def add_device(k, t):
        return t + got[k]

    total = lax.fori_loop(0, n_all, add_device, jnp.zeros((1, 128), F32), unroll=8)
    wide = jnp.broadcast_to(total, (8, 128))
    ratios = jnp.sqrt(pltpu.roll(wide, 120, 1) / (wide + 1.0))[0:1]
    ratios = jnp.where(lane < 8, ratios, 0.0)
    out_ratios[...] = ratios
    scale = []
    for b in range(blocks):
        r = jnp.sum(jnp.where(lane == layers[b], ratios, 0.0), keepdims=True)
        scale.append(jnp.where(lives[b] > 0, 0.1 * r, 0.0))
    out_scale[...] = per_row(scale)

    with jax.named_scope("drain"):
        wait_bytes(theirs, pair_send)
        wait_bytes(landed, link_send)
        wait_bytes(late, sum2_send)
        wait_bytes(others, sum_send)


def finish(upd, first, second, weights, scale, ratios, out_params, out_first, out_second, out_ratios, stage, sem):
    columns = stage.shape[1]
    step = columns // 4
    copies = [
        pltpu.make_async_copy(first, out_first, sem.at[0]),
        pltpu.make_async_copy(second, out_second, sem.at[1]),
    ]
    for c in copies:
        c.start()
    out_ratios[...] = ratios[:, : out_ratios.shape[1]]
    row_scale = scale[...]
    for n in range(4):

        def one(i, _, n=n):
            for k in range(4):
                cols = pl.ds(pl.multiple_of(n * step + i * 512 + k * 128, 128), 128)
                w = weights[0, :, cols].astype(F32)
                stage[:, cols] = (w - row_scale * upd[0, :, cols]).astype(BF16)
            return 0

        lax.fori_loop(0, step // 512, one, 0)
        cols = pl.ds(n * step, step)
        c = pltpu.make_async_copy(stage.at[:, cols], out_params.at[0, :, cols], sem.at[2 + n])
        c.start()
        copies.append(c)
    for c in copies:
        c.wait()


PARTS = 4


def shards(grad_parts, params, moment_first, moment_second, block_layer, block_valid, decay):
    rows, columns = params.shape[1:]
    n_section, n_shard = lax.axis_size("section"), lax.axis_size("shard")
    width = columns // 4
    chips = SIDE * SIDE
    hbm, vmem = pl.BlockSpec(memory_space=pltpu.HBM), pl.BlockSpec(memory_space=pltpu.VMEM)
    dma = pltpu.SemaphoreType.DMA
    groups = 9
    upd, first, second, weights, scale, ratios = pl.pallas_call(
        functools.partial(kernel, n_section, n_shard),
        out_shape=(
            pltpu.VMEM(moment_first.shape, F32),
            pltpu.VMEM(moment_first.shape, F32),
            pltpu.VMEM(moment_first.shape, F32),
            pltpu.VMEM(params.shape, BF16),
            pltpu.VMEM((rows, 128), F32),
            pltpu.VMEM((1, 128), F32),
        ),
        in_specs=[hbm] * 7,
        out_specs=(vmem,) * 6,
        scratch_shapes=[
            pltpu.VMEM((2, chips, rows, 2 * width), BF16),
            pltpu.VMEM((2, chips, rows, 2 * width), BF16),
            pltpu.VMEM((2, rows, 2 * width), BF16),
            pltpu.VMEM((4, SLOTS, rows, width), BF16),
            pltpu.VMEM((PARTS, 4, rows, width // PARTS), BF16),
            pltpu.SMEM(block_layer.shape, jnp.int32),
            pltpu.SMEM(block_valid.shape, jnp.int32),
            pltpu.SMEM(decay.shape, F32),
            pltpu.VMEM((1, 1, 128), F32),
            pltpu.VMEM((n_section * n_shard, 1, 128), F32),
            dma((groups,)),
            dma,
            dma((groups,)),
            dma,
            dma((4,)),
            dma((2, 4)),
            dma,
            dma,
            dma((PARTS,)),
            dma,
            dma((8,)),
            dma,
            dma,
        ],
        compiler_params=pltpu.CompilerParams(
            collective_id=0, has_side_effects=True, vmem_limit_bytes=48 * 2**20
        ),
        name="lamb_step",
    )(*(
        pltpu.with_memory_space_constraint(a, pltpu.HBM)
        for a in (grad_parts, params, moment_first, moment_second, block_layer, block_valid, decay)
    ))
    new_params, new_first, new_second, ratios = pl.pallas_call(
        finish,
        out_shape=(
            jax.ShapeDtypeStruct(params.shape, params.dtype),
            jax.ShapeDtypeStruct(moment_first.shape, F32),
            jax.ShapeDtypeStruct(moment_second.shape, F32),
            jax.ShapeDtypeStruct((1, decay.shape[0]), F32),
        ),
        in_specs=[vmem] * 6,
        out_specs=(hbm, hbm, hbm, vmem),
        scratch_shapes=[pltpu.VMEM((rows, columns), BF16), dma((6,))],
        compiler_params=pltpu.CompilerParams(vmem_limit_bytes=8 * 2**20),
        name="finish",
    )(upd, first, second, weights, scale, ratios)
    return new_params, new_first, new_second, ratios[0]


def solution(mesh):
    placed = (
        P("section", "shard", None, None),
        P("section", "shard", None),
        P("section", "shard", None),
        P("section", "shard", None),
        P("section", "shard"),
        P("section", "shard"),
        P(),
    )
    return jax.shard_map(
        shards,
        mesh=mesh,
        in_specs=placed,
        out_specs=(
            P("section", "shard", None),
            P("section", "shard", None),
            P("section", "shard", None),
            P(),
        ),
        check_vma=False,
    )
```

```python
import functools

import jax
import jax.numpy as jnp
from jax import lax
from jax.experimental import pallas as pl
from jax.experimental.pallas import tpu as pltpu
from jax.sharding import PartitionSpec as P

bias_first = 1.0 - 0.9**10
bias_second = 1.0 - 0.99**10

MESH = pl.DeviceIdType.MESH
F32, BF16 = jnp.float32, jnp.bfloat16
SIDE = 4
ORDER = (2, 1, 3, 0)
FAR, NEAR_OWN, NEAR_SUM = (0, 1, 2, 3), (4, 6, 8, 10), (5, 7, 9, 11)
FAR2, OWN2 = 12, 13
SLOTS = 14


def block_at(axis, main, other):
    return other * SIDE + main if axis == 0 else main * SIDE + other


def kernel(
    n_section, n_shard,
    grads, params, m_first, m_second, layer_hbm, valid_hbm, decay_hbm,
    upd, f_buf, s_buf, w_buf, out_scale, out_ratios,
    mine, theirs, ahead, landed, late, layer, valid, decay, sums, got,
    here_sem, pair_send, link_send, far_recv, near_recv, far2_recv, own2_recv, sum2_recv, sum2_send,
    start_recv, ahead_sem, small_sem, io_sem, sum_send, sum_recv,
):
    rows = w_buf.shape[1]
    columns = w_buf.shape[2]
    width = landed.shape[3]
    part = late.shape[3]
    parts = width // part
    section, shard = lax.axis_index("section"), lax.axis_index("shard")
    core, x, y = lax.rem(shard, 2), lax.rem(lax.div(shard, 2), SIDE), lax.div(shard, 2 * SIDE)
    me = section * n_shard + shard
    partner = shard + 1 - 2 * core

    def chip_at(dy, dx):
        return lax.rem(y + dy, SIDE) * SIDE + lax.rem(x + dx, SIDE)

    links = tuple(chip_at(dy, dx) * 2 + core for dy, dx in ((0, 1), (0, 3), (1, 0), (3, 0)))

    barrier = pltpu.get_barrier_semaphore()
    for peer in (partner,) + links:
        pl.semaphore_signal(barrier, inc=1, device_id={"shard": peer}, device_id_type=MESH)
    for k in range(1, n_section):
        pl.semaphore_signal(
            barrier, inc=1, device_id={"section": lax.rem(section + k, n_section)}, device_id_type=MESH
        )

    groups = []
    for j in ORDER:
        groups.append([(h, block_at(h, 2, j)) for h in (0, 1)])
    for j in ORDER:
        groups.append([(h, block_at(h, main, j)) for main in (1, 3, 0) for h in (0, 1)])
    group_of = {b: g for g, blocks in enumerate(groups) for b in blocks}

    def source(h, block, which):
        chip = chip_at(block // SIDE, block % SIDE)
        at = pl.multiple_of(chip * (2 * rows) + which * rows, rows)
        return grads.at[0, 0, pl.ds(at, rows), pl.ds(h * 2 * width, 2 * width)]

    def load(h, block):
        return pltpu.make_async_copy(
            source(h, block, core), mine.at[h, block], here_sem.at[group_of[h, block]]
        )

    def fetch_ahead(h):
        return pltpu.make_async_copy(source(h, block_at(h, 2, 2), 1 - core), ahead.at[h], ahead_sem)

    def pair(h, block):
        return pltpu.make_async_remote_copy(
            src_ref=source(h, block, 1 - core),
            dst_ref=theirs.at[h, block],
            send_sem=pair_send,
            recv_sem=here_sem.at[group_of[h, block]],
            device_id={"shard": partner},
            device_id_type=MESH,
        )

    size0 = width // PARTS0

    def pair0(p, h, q):
        cols = pl.ds(q * width + p * size0, size0)
        return pltpu.make_async_remote_copy(
            src_ref=ahead.at[h, :, cols],
            dst_ref=theirs.at[h, block_at(h, 2, 2), :, cols],
            send_sem=pair_send,
            recv_sem=start_recv.at[p],
            device_id={"shard": partner},
            device_id_type=MESH,
        )

    def wait_bytes(ref, sem):
        pltpu.make_async_copy(ref, ref, sem).wait()

    def quarter(ref, h, block, q):
        return ref.at[h, block, :, pl.ds(q * width, width)]

    def send(link, src, dst, recv_sem, send_sem=link_send):
        pltpu.make_async_remote_copy(
            src_ref=src,
            dst_ref=dst,
            send_sem=send_sem,
            recv_sem=recv_sem,
            device_id={"shard": links[link]},
            device_id_type=MESH,
        ).start()

    def add_up(dst, terms):
        size = dst.shape[1]
        step = min(512, size)

        def one(i, _):
            cols = pl.ds(pl.multiple_of(i * step, step), step)
            if len(terms) == 2:
                dst[:, cols] = terms[0][:, cols] + terms[1][:, cols]
            else:
                total = terms[0][:, cols].astype(F32)
                for t in terms[1:]:
                    total = total + t[:, cols].astype(F32)
                dst[:, cols] = total.astype(BF16)
            return 0

        lax.fori_loop(0, size // step, one, 0)

    for h in (0, 1):
        fetch_ahead(h).start()
        load(h, block_at(h, 2, 2)).start()
    for h, block in groups[1]:
        load(h, block).start()
    with jax.named_scope("barrier"):
        pl.semaphore_wait(barrier, 1 + len(links) + n_section - 1)
    wait_bytes(ahead, ahead_sem)
    for p in range(PARTS0):
        for h in (0, 1):
            for q in (0, 1):
                pair0(p, h, q).start()
    small = [
        pltpu.make_async_copy(a, b, small_sem.at[k])
        for k, (a, b) in enumerate(((layer_hbm, layer), (valid_hbm, valid), (decay_hbm, decay)))
    ]
    io = [
        pltpu.make_async_copy(params, w_buf, io_sem.at[0]),
        pltpu.make_async_copy(m_first, f_buf, io_sem.at[1]),
        pltpu.make_async_copy(m_second, s_buf, io_sem.at[1]),
    ]
    for g in range(1, len(groups)):
        for h, block in groups[g]:
            pair(h, block).start()
        if g > 1:
            for h, block in groups[g]:
                load(h, block).start()
        if g == 4:
            for c in small + io:
                c.start()

    ready = {0}

    def need(h, block):
        g = group_of[h, block]
        if g not in ready:
            ready.add(g)
            wait_bytes(mine.at[0, pl.ds(0, 2 * len(groups[g]))], here_sem.at[g])

    signs = (1, 3)
    each = [(axis, d, 2 * axis + d) for axis in (0, 1) for d in (0, 1)]
    four, eight = landed.at[0, pl.ds(0, 4)], landed.at[0, pl.ds(0, 8)]

    def own_terms(axis, block, q):
        need(axis, block)
        return [quarter(mine, axis, block, q), quarter(theirs, axis, block, q)]

    def far_first():
        wait_bytes(mine.at[0, pl.ds(0, 2)], here_sem.at[0])
        for p in range(PARTS0):
            wait_bytes(late.at[pl.ds(0, PARTS // PARTS0)], start_recv.at[p])
            for axis, d, link in each:
                here = pl.ds(p * size0, size0)
                terms = [t.at[:, here] for t in own_terms(axis, block_at(axis, 2, 2), d)]
                add_up(terms[0], terms)
                send(link, terms[0], landed.at[link, FAR[0], :, here], far_recv.at[0])

    def far(j):
        for axis, d, link in each:
            terms = own_terms(axis, block_at(axis, 2, ORDER[j]), d)
            add_up(terms[0], terms)
            send(link, terms[0], landed.at[link, FAR[j]], far_recv.at[j])

    def near_own(j):
        for axis, d, link in each:
            terms = own_terms(axis, block_at(axis, signs[d], ORDER[j]), 1 - d)
            add_up(terms[0], terms)
            send(link, terms[0], landed.at[link, NEAR_OWN[j]], near_recv.at[j])

    def near_sum(j):
        wait_bytes(four, far_recv.at[j])
        for axis, d, link in each:
            terms = own_terms(axis, block_at(axis, signs[d], ORDER[j]), d)
            add_up(terms[0], terms + [landed.at[link, FAR[j]]])
            send(link, terms[0], landed.at[link, NEAR_SUM[j]], near_recv.at[j])

    def first_axis(axis, j):
        block = block_at(axis, 0, ORDER[j])
        a, b = 2 * axis, 2 * axis + 1
        return [
            own_terms(axis, block, q)
            + [landed.at[(a, b)[q], NEAR_SUM[j]], landed.at[(b, a)[q], NEAR_OWN[j]]]
            for q in (0, 1)
        ]

    def settle(j):
        wait_bytes(eight, near_recv.at[j])
        for axis in (0, 1):
            for terms in first_axis(axis, j):
                add_up(terms[0], terms)

    def far2():
        settle(0)
        for axis, d, _ in each:
            link = 2 * (1 - axis) + d
            send(link, quarter(mine, axis, block_at(axis, 0, 2), d), landed.at[link, FAR2], far2_recv)

    def own2():
        settle(1)
        settle(2)
        for axis, d, _ in each:
            link = 2 * (1 - axis) + d
            src = quarter(mine, axis, block_at(axis, 0, signs[d]), 1 - d)
            send(link, src, landed.at[link, OWN2], own2_recv)

    def sum2():
        wait_bytes(four, far2_recv)
        for p in range(parts):
            for axis, d, _ in each:
                link = 2 * (1 - axis) + d
                at = pl.ds(p * part, part)
                dst = quarter(mine, axis, block_at(axis, 0, signs[d]), d).at[:, at]
                add_up(dst, [dst, landed.at[link, FAR2].at[:, at]])
                send(link, dst, late.at[p, link], sum2_recv.at[p], sum2_send)

    with jax.named_scope("far0"):
        far_first()
    for j in range(1, 4):
        with jax.named_scope(f"far{j}"):
            far(j)
    for j in range(3):
        with jax.named_scope(f"own{j}"):
            near_own(j)
        with jax.named_scope(f"sum{j}"):
            near_sum(j)
    near_own(3)

    for c in small + io[:1]:
        c.wait()
    wait_bytes(theirs.at[0, pl.ds(0, 8)], io_sem.at[1])
    row_block = lax.broadcasted_iota(jnp.int32, (rows, 128), 0) // 8
    lane = lax.broadcasted_iota(jnp.int32, (1, 128), 1)
    blocks = rows // 8

    def per_row(values):
        out = jnp.full((rows, 128), values[0])
        for b in range(1, blocks):
            out = jnp.where(row_block == b, values[b], out)
        return out

    layers = [layer[0, b] for b in range(blocks)]
    lives = [valid[0, b] for b in range(blocks)]
    row_decay = per_row([decay[l] for l in layers])
    row_live = per_row(lives) > 0

    row_layer = per_row(layers)
    row_lane = lax.broadcasted_iota(jnp.int32, (rows, 128), 1)
    own_lane = (row_lane == row_layer) & row_live
    own_lane_w = (row_lane == row_layer + 8) & row_live

    def by_layer(total, lanes):
        in_row = jnp.sum(total, axis=1, keepdims=True)
        return jnp.sum(jnp.where(lanes, in_row, 0.0), axis=0, keepdims=True)

    piece = 512

    def weights_sq(i, acc):
        for k in range(piece // 128):
            v = w_buf[0, :, pl.ds(pl.multiple_of(i * piece + k * 128, 128), 128)].astype(F32)
            acc = acc + v * v
        return acc

    w_sum = by_layer(lax.fori_loop(0, columns // piece, weights_sq, jnp.zeros((rows, 128), F32)), own_lane_w)

    with jax.named_scope("far2"):
        far2()
    with jax.named_scope("near_sum3"):
        near_sum(3)
    with jax.named_scope("own2"):
        own2()
    with jax.named_scope("sum2"):
        sum2()

    with jax.named_scope("early"):
        wait_bytes(eight, near_recv.at[3])
        for axis in (0, 1):
            both = first_axis(axis, 3)
            if axis == 0:
                wait_bytes(four, own2_recv)
            for q in (0, 1):
                terms = both[q] + [landed.at[2 * (1 - axis) + 1 - q, OWN2]]
                base = (2 * axis + q) * width

                def before(i, _, terms=terms, base=base):
                    at = pl.multiple_of(i * min(512, width), min(512, width))
                    here = pl.ds(at, min(512, width))
                    g = terms[0][:, here].astype(F32)
                    for t in terms[1:]:
                        g = g + t[:, here].astype(F32)
                    upd[0, :, pl.ds(base + at, min(512, width))] = g
                    return 0

                lax.fori_loop(0, width // min(512, width), before, 0)

    acc = jnp.zeros((rows, 128), F32)
    for p in range(parts):
        with jax.named_scope(f"late{p}"):
            wait_bytes(late.at[p], sum2_recv.at[p])
        for axis in (0, 1):
            for q in (0, 1):
                came = late.at[p, 2 * (1 - axis) + q]
                base = (2 * axis + q) * width + p * part
                step = min(512, part)

                def one(i, acc, came=came, base=base, step=step):
                    for k in range(step // 128):
                        at = i * step + k * 128
                        cols = pl.ds(pl.multiple_of(base + at, 128), 128)
                        g = upd[0, :, cols] + came[:, pl.ds(pl.multiple_of(at, 128), 128)].astype(F32)
                        old_f, old_s = f_buf[0, :, cols], s_buf[0, :, cols]
                        w = w_buf[0, :, cols].astype(F32)
                        first = 0.9 * old_f + 0.1 * g
                        second = 0.99 * old_s + 0.01 * g * g
                        u = (first * (1.0 / bias_first)) / (
                            jnp.sqrt(second * (1.0 / bias_second)) + 1e-06
                        ) + row_decay * w
                        upd[0, :, cols] = u
                        f_buf[0, :, cols] = jnp.where(row_live, first, old_f)
                        s_buf[0, :, cols] = jnp.where(row_live, second, old_s)
                        acc = acc + u * u
                    return acc

                acc = lax.fori_loop(0, part // step, one, acc)

    vec = by_layer(acc, own_lane) + w_sum
    sums[0] = vec
    got[me] = vec

    def tell(to_section, to_shard):
        pltpu.make_async_remote_copy(
            src_ref=sums.at[0],
            dst_ref=got.at[me],
            send_sem=sum_send,
            recv_sem=sum_recv,
            device_id={"section": to_section, "shard": to_shard},
            device_id_type=MESH,
        ).start()

    far_from = (0, 1, 2, 1)
    away = sorted(
        ((ds, dy, dx, c) for ds in range(n_section) for dy in range(SIDE) for dx in range(SIDE) for c in (0, 1)),
        key=lambda a: -sum(far_from[k] for k in a[:3]) - a[3] / 2,
    )
    sections = [lax.rem(section + k, n_section) for k in range(n_section)]
    shards_at = {
        (dy, dx, c): chip_at(dy, dx) * 2 + (core if c == 0 else 1 - core)
        for dy in range(SIDE) for dx in range(SIDE) for c in (0, 1)
    }
    with jax.named_scope("tell"):
        for ds, dy, dx, c in away[:-1]:
            tell(sections[ds], shards_at[dy, dx, c])
    n_all = n_section * n_shard
    others = got.at[pl.ds(0, n_all - 1)]
    with jax.named_scope("everyone"):
        wait_bytes(others, sum_recv)

    def add_device(k, t):
        return t + got[k]

    total = lax.fori_loop(0, n_all, add_device, jnp.zeros((1, 128), F32), unroll=8)
    wide = jnp.broadcast_to(total, (8, 128))
    ratios = jnp.sqrt(pltpu.roll(wide, 120, 1) / (wide + 1.0))[0:1]
    ratios = jnp.where(lane < 8, ratios, 0.0)
    out_ratios[...] = ratios
    row_ratio = jnp.sum(jnp.where(own_lane, ratios, 0.0), axis=1, keepdims=True)
    out_scale[...] = jnp.broadcast_to(0.1 * row_ratio, (rows, 128))

    with jax.named_scope("drain"):
        wait_bytes(theirs, pair_send)
        wait_bytes(landed, link_send)
        wait_bytes(late, sum2_send)
        wait_bytes(others, sum_send)


def finish(upd, first, second, weights, scale, ratios, out_params, out_first, out_second, out_ratios, stage, ratio, sem):
    columns = stage.shape[1]
    step = columns // 4
    copies = [
        pltpu.make_async_copy(first, out_first, sem.at[0]),
        pltpu.make_async_copy(second, out_second, sem.at[1]),
    ]
    ratio[...] = ratios[:, : ratio.shape[1]]
    copies.append(pltpu.make_async_copy(ratio, out_ratios, sem.at[6]))
    for c in copies:
        c.start()
    row_scale = scale[...]
    for n in range(4):
      with jax.named_scope(f"fin{n}"):

        def one(i, _, n=n):
            for k in range(4):
                cols = pl.ds(pl.multiple_of(n * step + i * 512 + k * 128, 128), 128)
                w = weights[0, :, cols].astype(F32)
                stage[:, cols] = (w - row_scale * upd[0, :, cols]).astype(BF16)
            return 0

        lax.fori_loop(0, step // 512, one, 0)
        cols = pl.ds(n * step, step)
        c = pltpu.make_async_copy(stage.at[:, cols], out_params.at[0, :, cols], sem.at[2 + n])
        c.start()
        copies.append(c)
    with jax.named_scope("finw"):
      for c in copies:
        c.wait()


PARTS = 4
PARTS0 = 4


def shards(grad_parts, params, moment_first, moment_second, block_layer, block_valid, decay):
    rows, columns = params.shape[1:]
    n_section, n_shard = lax.axis_size("section"), lax.axis_size("shard")
    width = columns // 4
    chips = SIDE * SIDE
    hbm, vmem = pl.BlockSpec(memory_space=pltpu.HBM), pl.BlockSpec(memory_space=pltpu.VMEM)
    dma = pltpu.SemaphoreType.DMA
    groups = 8
    upd, first, second, weights, scale, ratios = pl.pallas_call(
        functools.partial(kernel, n_section, n_shard),
        out_shape=(
            pltpu.VMEM(moment_first.shape, F32),
            pltpu.VMEM(moment_first.shape, F32),
            pltpu.VMEM(moment_first.shape, F32),
            pltpu.VMEM(params.shape, BF16),
            pltpu.VMEM((rows, 128), F32),
            pltpu.VMEM((1, 128), F32),
        ),
        in_specs=[hbm] * 7,
        out_specs=(vmem,) * 6,
        scratch_shapes=[
            pltpu.VMEM((2, chips, rows, 2 * width), BF16),
            pltpu.VMEM((2, chips, rows, 2 * width), BF16),
            pltpu.VMEM((2, rows, 2 * width), BF16),
            pltpu.VMEM((4, SLOTS, rows, width), BF16),
            pltpu.VMEM((PARTS, 4, rows, width // PARTS), BF16),
            pltpu.SMEM(block_layer.shape, jnp.int32),
            pltpu.SMEM(block_valid.shape, jnp.int32),
            pltpu.SMEM(decay.shape, F32),
            pltpu.VMEM((1, 1, 128), F32),
            pltpu.VMEM((n_section * n_shard, 1, 128), F32),
            dma((groups,)),
            dma,
            dma,
            dma((4,)),
            dma((4,)),
            dma,
            dma,
            dma((PARTS,)),
            dma,
            dma((PARTS0,)),
            dma,
            dma((3,)),
            dma((2,)),
            dma,
            dma,
        ],
        compiler_params=pltpu.CompilerParams(
            collective_id=0, has_side_effects=True, vmem_limit_bytes=48 * 2**20
        ),
        name="lamb_step",
    )(*(
        pltpu.with_memory_space_constraint(a, pltpu.HBM)
        for a in (grad_parts, params, moment_first, moment_second, block_layer, block_valid, decay)
    ))
    new_params, new_first, new_second, ratios = pl.pallas_call(
        finish,
        out_shape=(
            jax.ShapeDtypeStruct(params.shape, params.dtype),
            jax.ShapeDtypeStruct(moment_first.shape, F32),
            jax.ShapeDtypeStruct(moment_second.shape, F32),
            jax.ShapeDtypeStruct((1, decay.shape[0]), F32),
        ),
        in_specs=[vmem] * 6,
        out_specs=(hbm,) * 4,
        scratch_shapes=[pltpu.VMEM((rows, columns), BF16), pltpu.VMEM((1, decay.shape[0]), F32), dma((7,))],
        compiler_params=pltpu.CompilerParams(vmem_limit_bytes=8 * 2**20),
        name="finish",
    )(upd, first, second, weights, scale, ratios)
    return new_params, new_first, new_second, ratios[0]


def solution(mesh):
    placed = (
        P("section", "shard", None, None),
        P("section", "shard", None),
        P("section", "shard", None),
        P("section", "shard", None),
        P("section", "shard"),
        P("section", "shard"),
        P(),
    )
    return jax.shard_map(
        shards,
        mesh=mesh,
        in_specs=placed,
        out_specs=(
            P("section", "shard", None),
            P("section", "shard", None),
            P("section", "shard", None),
            P(),
        ),
        check_vma=False,
    )
```

```python
import functools

import jax
import jax.numpy as jnp
from jax import lax
from jax.experimental import pallas as pl
from jax.experimental.pallas import tpu as pltpu
from jax.sharding import PartitionSpec as P

bias_first = 1.0 - 0.9**10
bias_second = 1.0 - 0.99**10

MESH = pl.DeviceIdType.MESH
F32, BF16 = jnp.float32, jnp.bfloat16
SIDE = 4
ORDER = (2, 1, 3, 0)
FAR, NEAR_OWN, NEAR_SUM = (0, 1, 2, 3), (4, 6, 8, 10), (5, 7, 9, 11)
FAR2, OWN2 = 12, 13
SLOTS = 14


def block_at(axis, main, other):
    return other * SIDE + main if axis == 0 else main * SIDE + other


def kernel(
    n_section, n_shard,
    grads, params, m_first, m_second, layer_hbm, valid_hbm, decay_hbm,
    upd, f_buf, s_buf, w_buf, out_mask, got,
    mine, theirs, ahead, landed, late, layer, valid, decay, sums,
    here_sem, pair_send, link_send, far_recv, near_recv, far2_recv, own2_recv, sum2_recv, sum2_send,
    start_recv, ahead_sem, small_sem, io_sem, sum_send, sum_recv,
):
    rows = w_buf.shape[1]
    columns = w_buf.shape[2]
    width = landed.shape[3]
    parts = [(sum(PARTS[:p]) * (width // 16), PARTS[p] * (width // 16)) for p in range(len(PARTS))]
    section, shard = lax.axis_index("section"), lax.axis_index("shard")
    core, x, y = lax.rem(shard, 2), lax.rem(lax.div(shard, 2), SIDE), lax.div(shard, 2 * SIDE)
    me = section * n_shard + shard
    partner = shard + 1 - 2 * core

    def chip_at(dy, dx):
        return lax.rem(y + dy, SIDE) * SIDE + lax.rem(x + dx, SIDE)

    links = tuple(chip_at(dy, dx) * 2 + core for dy, dx in ((0, 1), (0, 3), (1, 0), (3, 0)))

    barrier = pltpu.get_barrier_semaphore()
    for peer in (partner,) + links:
        pl.semaphore_signal(barrier, inc=1, device_id={"shard": peer}, device_id_type=MESH)
    for k in range(1, n_section):
        pl.semaphore_signal(
            barrier, inc=1, device_id={"section": lax.rem(section + k, n_section)}, device_id_type=MESH
        )

    groups = []
    for j in ORDER:
        groups.append([(h, block_at(h, 2, j)) for h in (0, 1)])
    for j in ORDER:
        groups.append([(h, block_at(h, main, j)) for main in (1, 3, 0) for h in (0, 1)])
    group_of = {b: g for g, blocks in enumerate(groups) for b in blocks}

    def source(h, block, which):
        chip = chip_at(block // SIDE, block % SIDE)
        at = pl.multiple_of(chip * (2 * rows) + which * rows, rows)
        return grads.at[0, 0, pl.ds(at, rows), pl.ds(h * 2 * width, 2 * width)]

    def load(h, block):
        return pltpu.make_async_copy(
            source(h, block, core), mine.at[h, block], here_sem.at[group_of[h, block]]
        )

    def fetch_ahead(h):
        return pltpu.make_async_copy(source(h, block_at(h, 2, 2), 1 - core), ahead.at[h], ahead_sem)

    def pair(h, block):
        return pltpu.make_async_remote_copy(
            src_ref=source(h, block, 1 - core),
            dst_ref=theirs.at[h, block],
            send_sem=pair_send,
            recv_sem=here_sem.at[group_of[h, block]],
            device_id={"shard": partner},
            device_id_type=MESH,
        )

    size0 = width // PARTS0

    def pair0(p, h, q):
        cols = pl.ds(q * width + p * size0, size0)
        return pltpu.make_async_remote_copy(
            src_ref=ahead.at[h, :, cols],
            dst_ref=theirs.at[h, block_at(h, 2, 2), :, cols],
            send_sem=pair_send,
            recv_sem=start_recv.at[p],
            device_id={"shard": partner},
            device_id_type=MESH,
        )

    def wait_bytes(ref, sem):
        pltpu.make_async_copy(ref, ref, sem).wait()

    def quarter(ref, h, block, q):
        return ref.at[h, block, :, pl.ds(q * width, width)]

    def send(link, src, dst, recv_sem, send_sem=link_send):
        pltpu.make_async_remote_copy(
            src_ref=src,
            dst_ref=dst,
            send_sem=send_sem,
            recv_sem=recv_sem,
            device_id={"shard": links[link]},
            device_id_type=MESH,
        ).start()

    def add_up(dst, terms):
        size = dst.shape[1]
        step = min(512, size)

        def one(i, _):
            cols = pl.ds(pl.multiple_of(i * step, step), step)
            if len(terms) == 2:
                dst[:, cols] = terms[0][:, cols] + terms[1][:, cols]
            else:
                total = terms[0][:, cols].astype(F32)
                for t in terms[1:]:
                    total = total + t[:, cols].astype(F32)
                dst[:, cols] = total.astype(BF16)
            return 0

        lax.fori_loop(0, size // step, one, 0)

    for h in (0, 1):
        fetch_ahead(h).start()
        load(h, block_at(h, 2, 2)).start()
    for h, block in groups[1]:
        load(h, block).start()
    with jax.named_scope("barrier"):
        pl.semaphore_wait(barrier, 1 + len(links) + n_section - 1)
    wait_bytes(ahead, ahead_sem)
    for p in range(PARTS0):
        for h in (0, 1):
            for q in (0, 1):
                pair0(p, h, q).start()
    small = [
        pltpu.make_async_copy(a, b, small_sem.at[k])
        for k, (a, b) in enumerate(((layer_hbm, layer), (valid_hbm, valid), (decay_hbm, decay)))
    ]
    io = [
        pltpu.make_async_copy(params, w_buf, io_sem.at[0]),
        pltpu.make_async_copy(m_first, f_buf, io_sem.at[1]),
        pltpu.make_async_copy(m_second, s_buf, io_sem.at[1]),
    ]
    for g in range(1, len(groups)):
        for h, block in groups[g]:
            pair(h, block).start()
        if g > 1:
            for h, block in groups[g]:
                load(h, block).start()
        if g == 4:
            for c in small + io:
                c.start()

    ready = {0}

    def need(h, block):
        g = group_of[h, block]
        if g not in ready:
            ready.add(g)
            wait_bytes(mine.at[0, pl.ds(0, 2 * len(groups[g]))], here_sem.at[g])

    signs = (1, 3)
    each = [(axis, d, 2 * axis + d) for axis in (0, 1) for d in (0, 1)]
    four, eight = landed.at[0, pl.ds(0, 4)], landed.at[0, pl.ds(0, 8)]

    def own_terms(axis, block, q):
        need(axis, block)
        return [quarter(mine, axis, block, q), quarter(theirs, axis, block, q)]

    def far_first():
        wait_bytes(mine.at[0, pl.ds(0, 2)], here_sem.at[0])
        for p in range(PARTS0):
            wait_bytes(ahead.at[0, :, pl.ds(0, 4 * size0)], start_recv.at[p])
            for axis, d, link in each:
                here = pl.ds(p * size0, size0)
                terms = [t.at[:, here] for t in own_terms(axis, block_at(axis, 2, 2), d)]
                add_up(terms[0], terms)
                send(link, terms[0], landed.at[link, FAR[0], :, here], far_recv.at[0])

    def far(j):
        for axis, d, link in each:
            terms = own_terms(axis, block_at(axis, 2, ORDER[j]), d)
            add_up(terms[0], terms)
            send(link, terms[0], landed.at[link, FAR[j]], far_recv.at[j])

    def near_own(j):
        for axis, d, link in each:
            terms = own_terms(axis, block_at(axis, signs[d], ORDER[j]), 1 - d)
            add_up(terms[0], terms)
            send(link, terms[0], landed.at[link, NEAR_OWN[j]], near_recv.at[j])

    def near_sum(j):
        wait_bytes(four, far_recv.at[j])
        for axis, d, link in each:
            terms = own_terms(axis, block_at(axis, signs[d], ORDER[j]), d)
            add_up(terms[0], terms + [landed.at[link, FAR[j]]])
            send(link, terms[0], landed.at[link, NEAR_SUM[j]], near_recv.at[j])

    def first_axis(axis, j):
        block = block_at(axis, 0, ORDER[j])
        a, b = 2 * axis, 2 * axis + 1
        return [
            own_terms(axis, block, q)
            + [landed.at[(a, b)[q], NEAR_SUM[j]], landed.at[(b, a)[q], NEAR_OWN[j]]]
            for q in (0, 1)
        ]

    def settle(j):
        wait_bytes(eight, near_recv.at[j])
        for axis in (0, 1):
            for terms in first_axis(axis, j):
                add_up(terms[0], terms)

    def far2():
        settle(0)
        for axis, d, _ in each:
            link = 2 * (1 - axis) + d
            send(link, quarter(mine, axis, block_at(axis, 0, 2), d), landed.at[link, FAR2], far2_recv)

    def own2():
        settle(1)
        settle(2)
        for axis, d, _ in each:
            link = 2 * (1 - axis) + d
            src = quarter(mine, axis, block_at(axis, 0, signs[d]), 1 - d)
            send(link, src, landed.at[link, OWN2], own2_recv)

    def sum2():
        wait_bytes(four, far2_recv)
        for p, (start, size) in enumerate(parts):
            for axis, d, _ in each:
                link = 2 * (1 - axis) + d
                at = pl.ds(start, size)
                dst = quarter(mine, axis, block_at(axis, 0, signs[d]), d).at[:, at]
                add_up(dst, [dst, landed.at[link, FAR2].at[:, at]])
                send(link, dst, late.at[link, :, at], sum2_recv.at[p], sum2_send)

    with jax.named_scope("far0"):
        far_first()
    for j in range(1, 4):
        with jax.named_scope(f"far{j}"):
            far(j)
    for j in range(3):
        with jax.named_scope(f"own{j}"):
            near_own(j)
        with jax.named_scope(f"sum{j}"):
            near_sum(j)
    near_own(3)

    for c in small + io[:1]:
        c.wait()
    wait_bytes(theirs.at[0, pl.ds(0, 8)], io_sem.at[1])
    row_block = lax.broadcasted_iota(jnp.int32, (rows, 128), 0) // 8
    blocks = rows // 8

    def per_row(values):
        out = jnp.full((rows, 128), values[0])
        for b in range(1, blocks):
            out = jnp.where(row_block == b, values[b], out)
        return out

    layers = [layer[0, b] for b in range(blocks)]
    lives = [valid[0, b] for b in range(blocks)]
    row_decay = per_row([decay[l] for l in layers])
    row_live = per_row(lives) > 0

    row_layer = per_row(layers)
    row_lane = lax.broadcasted_iota(jnp.int32, (rows, 128), 1)
    own_lane = (row_lane == row_layer) & row_live
    own_lane_w = (row_lane == row_layer + 8) & row_live
    out_mask[...] = jnp.where(own_lane, 1.0, 0.0)

    def by_layer(total, lanes):
        in_row = jnp.sum(total, axis=1, keepdims=True)
        return jnp.sum(jnp.where(lanes, in_row, 0.0), axis=0, keepdims=True)

    piece = 512

    def weights_sq(i, acc):
        for k in range(piece // 128):
            v = w_buf[0, :, pl.ds(pl.multiple_of(i * piece + k * 128, 128), 128)].astype(F32)
            acc = acc + v * v
        return acc

    w_sum = by_layer(lax.fori_loop(0, columns // piece, weights_sq, jnp.zeros((rows, 128), F32)), own_lane_w)

    with jax.named_scope("far2"):
        far2()
    with jax.named_scope("near_sum3"):
        near_sum(3)
    with jax.named_scope("own2"):
        own2()
    with jax.named_scope("sum2"):
        sum2()

    with jax.named_scope("early"):
        wait_bytes(eight, near_recv.at[3])
        for axis in (0, 1):
            both = first_axis(axis, 3)
            if axis == 0:
                wait_bytes(four, own2_recv)
            for q in (0, 1):
                terms = both[q] + [landed.at[2 * (1 - axis) + 1 - q, OWN2]]
                base = (2 * axis + q) * width

                def before(i, _, terms=terms, base=base):
                    at = pl.multiple_of(i * min(512, width), min(512, width))
                    here = pl.ds(at, min(512, width))
                    g = terms[0][:, here].astype(F32)
                    for t in terms[1:]:
                        g = g + t[:, here].astype(F32)
                    upd[0, :, pl.ds(base + at, min(512, width))] = g
                    return 0

                lax.fori_loop(0, width // min(512, width), before, 0)

    acc = jnp.zeros((rows, 128), F32)
    for p, (start, part) in enumerate(parts):
        with jax.named_scope(f"late{p}"):
            wait_bytes(late.at[:, :, pl.ds(start, part)], sum2_recv.at[p])
        for axis in (0, 1):
            for q in (0, 1):
                came = late.at[2 * (1 - axis) + q, :, pl.ds(start, part)]
                base = (2 * axis + q) * width + start
                step = min(512, part)

                def one(i, acc, came=came, base=base, step=step):
                    for k in range(step // 128):
                        at = i * step + k * 128
                        cols = pl.ds(pl.multiple_of(base + at, 128), 128)
                        g = upd[0, :, cols] + came[:, pl.ds(pl.multiple_of(at, 128), 128)].astype(F32)
                        old_f, old_s = f_buf[0, :, cols], s_buf[0, :, cols]
                        w = w_buf[0, :, cols].astype(F32)
                        first = 0.9 * old_f + 0.1 * g
                        second = 0.99 * old_s + 0.01 * g * g
                        u = (first * (1.0 / bias_first)) / (
                            jnp.sqrt(second * (1.0 / bias_second)) + 1e-06
                        ) + row_decay * w
                        upd[0, :, cols] = u
                        f_buf[0, :, cols] = jnp.where(row_live, first, old_f)
                        s_buf[0, :, cols] = jnp.where(row_live, second, old_s)
                        acc = acc + u * u
                    return acc

                acc = lax.fori_loop(0, part // step, one, acc)

    vec = by_layer(acc, own_lane) + w_sum
    sums[0] = vec
    got[me] = vec

    def tell(to_section, to_shard):
        pltpu.make_async_remote_copy(
            src_ref=sums.at[0],
            dst_ref=got.at[me],
            send_sem=sum_send,
            recv_sem=sum_recv,
            device_id={"section": to_section, "shard": to_shard},
            device_id_type=MESH,
        ).start()

    far_from = (0, 1, 2, 1)
    away = sorted(
        ((ds, dy, dx, c) for ds in range(n_section) for dy in range(SIDE) for dx in range(SIDE) for c in (0, 1)),
        key=lambda a: -sum(far_from[k] for k in a[:3]) - a[3] / 2,
    )
    sections = [lax.rem(section + k, n_section) for k in range(n_section)]
    shards_at = {
        (dy, dx, c): chip_at(dy, dx) * 2 + (core if c == 0 else 1 - core)
        for dy in range(SIDE) for dx in range(SIDE) for c in (0, 1)
    }
    with jax.named_scope("tell"):
        for ds, dy, dx, c in away[:-1]:
            tell(sections[ds], shards_at[dy, dx, c])
    n_all = n_section * n_shard
    others = got.at[pl.ds(0, n_all - 1)]
    with jax.named_scope("everyone"):
        wait_bytes(others, sum_recv)

    with jax.named_scope("drain"):
        wait_bytes(theirs, pair_send)
        wait_bytes(landed, link_send)
        wait_bytes(late, sum2_send)
        wait_bytes(others, sum_send)


def finish(upd, first, second, weights, mask, got, out_params, out_first, out_second, out_ratios, stage, ratio, sem):
    columns = stage.shape[1]
    step = columns // 4
    copies = [
        pltpu.make_async_copy(first, out_first, sem.at[0]),
        pltpu.make_async_copy(second, out_second, sem.at[1]),
    ]
    for c in copies:
        c.start()
    several = [got[k] for k in range(8)]
    for k in range(8, got.shape[0]):
        several[k % 8] = several[k % 8] + got[k]
    while len(several) > 1:
        several = [a + b for a, b in zip(several[::2], several[1::2])]
    wide = jnp.broadcast_to(several[0], (8, 128))
    lane = lax.broadcasted_iota(jnp.int32, (1, 128), 1)
    ratios = jnp.sqrt(pltpu.roll(wide, 120, 1) / (wide + 1.0))[0:1]
    ratios = jnp.where(lane < ratio.shape[1], ratios, 0.0)
    ratio[...] = ratios[:, : ratio.shape[1]]
    c = pltpu.make_async_copy(ratio, out_ratios, sem.at[6])
    c.start()
    copies.append(c)
    row_ratio = jnp.sum(jnp.where(mask[...] > 0.5, ratios, 0.0), axis=1, keepdims=True)
    row_scale = jnp.broadcast_to(0.1 * row_ratio, mask.shape)
    for n in range(4):
      with jax.named_scope(f"fin{n}"):

        def one(i, _, n=n):
            for k in range(4):
                cols = pl.ds(pl.multiple_of(n * step + i * 512 + k * 128, 128), 128)
                w = weights[0, :, cols].astype(F32)
                stage[:, cols] = (w - row_scale * upd[0, :, cols]).astype(BF16)
            return 0

        lax.fori_loop(0, step // 512, one, 0)
        cols = pl.ds(n * step, step)
        c = pltpu.make_async_copy(stage.at[:, cols], out_params.at[0, :, cols], sem.at[2 + n])
        c.start()
        copies.append(c)
    with jax.named_scope("finw"):
      for c in copies:
        c.wait()


PARTS = (8, 4, 2, 2)
PARTS0 = 4


def shards(grad_parts, params, moment_first, moment_second, block_layer, block_valid, decay):
    rows, columns = params.shape[1:]
    n_section, n_shard = lax.axis_size("section"), lax.axis_size("shard")
    width = columns // 4
    chips = SIDE * SIDE
    hbm, vmem = pl.BlockSpec(memory_space=pltpu.HBM), pl.BlockSpec(memory_space=pltpu.VMEM)
    dma = pltpu.SemaphoreType.DMA
    groups = 8
    upd, first, second, weights, mask, got = pl.pallas_call(
        functools.partial(kernel, n_section, n_shard),
        out_shape=(
            pltpu.VMEM(moment_first.shape, F32),
            pltpu.VMEM(moment_first.shape, F32),
            pltpu.VMEM(moment_first.shape, F32),
            pltpu.VMEM(params.shape, BF16),
            pltpu.VMEM((rows, 128), F32),
            pltpu.VMEM((n_section * n_shard, 1, 128), F32),
        ),
        in_specs=[hbm] * 7,
        out_specs=(vmem,) * 6,
        scratch_shapes=[
            pltpu.VMEM((2, chips, rows, 2 * width), BF16),
            pltpu.VMEM((2, chips, rows, 2 * width), BF16),
            pltpu.VMEM((2, rows, 2 * width), BF16),
            pltpu.VMEM((4, SLOTS, rows, width), BF16),
            pltpu.VMEM((4, rows, width), BF16),
            pltpu.SMEM(block_layer.shape, jnp.int32),
            pltpu.SMEM(block_valid.shape, jnp.int32),
            pltpu.SMEM(decay.shape, F32),
            pltpu.VMEM((1, 1, 128), F32),
            dma((groups,)),
            dma,
            dma,
            dma((4,)),
            dma((4,)),
            dma,
            dma,
            dma((len(PARTS),)),
            dma,
            dma((PARTS0,)),
            dma,
            dma((3,)),
            dma((2,)),
            dma,
            dma,
        ],
        compiler_params=pltpu.CompilerParams(
            collective_id=0, has_side_effects=True, vmem_limit_bytes=48 * 2**20
        ),
        name="lamb_step",
    )(*(
        pltpu.with_memory_space_constraint(a, pltpu.HBM)
        for a in (grad_parts, params, moment_first, moment_second, block_layer, block_valid, decay)
    ))
    new_params, new_first, new_second, ratios = pl.pallas_call(
        finish,
        out_shape=(
            jax.ShapeDtypeStruct(params.shape, params.dtype),
            jax.ShapeDtypeStruct(moment_first.shape, F32),
            jax.ShapeDtypeStruct(moment_second.shape, F32),
            jax.ShapeDtypeStruct((1, decay.shape[0]), F32),
        ),
        in_specs=[vmem] * 6,
        out_specs=(hbm,) * 4,
        scratch_shapes=[pltpu.VMEM((rows, columns), BF16), pltpu.VMEM((1, decay.shape[0]), F32), dma((7,))],
        compiler_params=pltpu.CompilerParams(vmem_limit_bytes=8 * 2**20),
        name="finish",
    )(upd, first, second, weights, mask, got)
    return new_params, new_first, new_second, ratios[0]


def solution(mesh):
    placed = (
        P("section", "shard", None, None),
        P("section", "shard", None),
        P("section", "shard", None),
        P("section", "shard", None),
        P("section", "shard"),
        P("section", "shard"),
        P(),
    )
    return jax.shard_map(
        shards,
        mesh=mesh,
        in_specs=placed,
        out_specs=(
            P("section", "shard", None),
            P("section", "shard", None),
            P("section", "shard", None),
            P(),
        ),
        check_vma=False,
    )
```

```python
import functools

import jax
import jax.numpy as jnp
from jax import lax
from jax.experimental import pallas as pl
from jax.experimental.pallas import tpu as pltpu
from jax.sharding import PartitionSpec as P

bias_first = 1.0 - 0.9**10
bias_second = 1.0 - 0.99**10

MESH = pl.DeviceIdType.MESH
F32, BF16 = jnp.float32, jnp.bfloat16
SIDE = 4
ORDER = (2, 1, 3, 0)
FAR, NEAR_OWN, NEAR_SUM = (0, 1, 2, 3), (4, 6, 8, 10), (5, 7, 9, 11)
FAR2, OWN2 = 12, 13
SLOTS = 14


def block_at(axis, main, other):
    return other * SIDE + main if axis == 0 else main * SIDE + other


def kernel(
    n_section, n_shard,
    grads, params, m_first, m_second, layer_hbm, valid_hbm, decay_hbm,
    upd, f_buf, s_buf, w_buf, out_mask, got,
    mine, theirs, ahead, landed, late, layer, valid, decay, sums,
    here_sem, pair_send, link_send, far_recv, near_recv, far2_recv, own2_recv, own2_send, sum2_recv, sum2_send,
    start_recv, heard, near_in, roots_in, all_in, go_on, ahead_sem, small_sem, io_sem, sum_send, sum_recv,
):
    rows = w_buf.shape[1]
    columns = w_buf.shape[2]
    width = landed.shape[3]
    parts = [(sum(PARTS[:p]) * (width // 16), PARTS[p] * (width // 16)) for p in range(len(PARTS))]
    section, shard = lax.axis_index("section"), lax.axis_index("shard")
    core, x, y = lax.rem(shard, 2), lax.rem(lax.div(shard, 2), SIDE), lax.div(shard, 2 * SIDE)
    me = section * n_shard + shard
    partner = shard + 1 - 2 * core

    def chip_at(dy, dx):
        return lax.rem(y + dy, SIDE) * SIDE + lax.rem(x + dx, SIDE)

    links = tuple(chip_at(dy, dx) * 2 + core for dy, dx in ((0, 1), (0, 3), (1, 0), (3, 0)))

    root = (core == 1) & (x == 0) & (y == 0)

    def to_shards(sem, peers):
        for peer in peers:
            pl.semaphore_signal(sem, inc=1, device_id={"shard": peer}, device_id_type=MESH)

    def to_roots(sem):
        for k in range(1, n_section):
            pl.semaphore_signal(
                sem, inc=1, device_id={"section": lax.rem(section + k, n_section)}, device_id_type=MESH
            )

    barrier = pltpu.get_barrier_semaphore()
    to_shards(barrier, (partner,))

    @pl.when(core == 1)
    def _():
        to_shards(barrier, links)

    @pl.when(root)
    def _():
        to_roots(barrier)

    def hear(k):
        @pl.when(core == 1)
        def _():
            pl.semaphore_wait(heard.at[k], len(links))
            if k + 1 < ROUNDS:
                to_shards(heard.at[k + 1], links)
            if k == 0:
                to_shards(near_in, (partner,))

        if k + 1 == ROUNDS:

            @pl.when(root)
            def _():
                to_roots(roots_in)

    def hear_roots():
        @pl.when(root)
        def _():
            pl.semaphore_wait(roots_in, n_section - 1)
            to_shards(all_in, [k for k in range(n_shard) if k != 1])

    groups = []
    for j in ORDER:
        groups.append([(h, block_at(h, 2, j)) for h in (0, 1)])
    for j in ORDER:
        groups.append([(h, block_at(h, main, j)) for main in (1, 3, 0) for h in (0, 1)])
    group_of = {b: g for g, blocks in enumerate(groups) for b in blocks}

    size0 = width // PARTS0
    first4 = [(h, q) for h in (0, 1) for q in (0, 1)]

    def source(h, block, which):
        chip = chip_at(block // SIDE, block % SIDE)
        at = pl.multiple_of(chip * (2 * rows) + which * rows, rows)
        return grads.at[0, 0, pl.ds(at, rows), pl.ds(h * 2 * width, 2 * width)]

    def load(h, block):
        return pltpu.make_async_copy(
            source(h, block, core), mine.at[h, block], here_sem.at[group_of[h, block]]
        )

    def fetch_ahead(p, h, q):
        cols = pl.ds(q * width + p * size0, size0)
        return pltpu.make_async_copy(
            source(h, block_at(h, 2, 2), 1 - core).at[:, cols], ahead.at[h, :, cols], ahead_sem.at[p]
        )

    def pair(h, block):
        return pltpu.make_async_remote_copy(
            src_ref=source(h, block, 1 - core),
            dst_ref=theirs.at[h, block],
            send_sem=pair_send,
            recv_sem=here_sem.at[group_of[h, block]],
            device_id={"shard": partner},
            device_id_type=MESH,
        )

    def pair0(p, h, q):
        cols = pl.ds(q * width + p * size0, size0)
        return pltpu.make_async_remote_copy(
            src_ref=ahead.at[h, :, cols],
            dst_ref=theirs.at[h, block_at(h, 2, 2), :, cols],
            send_sem=pair_send,
            recv_sem=start_recv.at[p],
            device_id={"shard": partner},
            device_id_type=MESH,
        )

    def wait_bytes(ref, sem):
        pltpu.make_async_copy(ref, ref, sem).wait()

    def quarter(ref, h, block, q):
        return ref.at[h, block, :, pl.ds(q * width, width)]

    def send(link, src, dst, recv_sem, send_sem=link_send):
        pltpu.make_async_remote_copy(
            src_ref=src,
            dst_ref=dst,
            send_sem=send_sem,
            recv_sem=recv_sem,
            device_id={"shard": links[link]},
            device_id_type=MESH,
        ).start()

    def add_up(dst, terms):
        size = dst.shape[1]
        step = min(512, size)
        assert size % step == 0

        def one(i, _):
            cols = pl.ds(pl.multiple_of(i * step, step), step)
            if len(terms) == 2:
                dst[:, cols] = terms[0][:, cols] + terms[1][:, cols]
            else:
                total = terms[0][:, cols].astype(F32)
                for t in terms[1:]:
                    total = total + t[:, cols].astype(F32)
                dst[:, cols] = total.astype(BF16)
            return 0

        lax.fori_loop(0, size // step, one, 0)

    for p in range(PARTS0):
        for h, q in first4:
            fetch_ahead(p, h, q).start()
        if p == 0:
            for h in (0, 1):
                load(h, block_at(h, 2, 2)).start()
    for h, block in groups[1]:
        load(h, block).start()
    with jax.named_scope("barrier"):
        @pl.when(core == 0)
        def _():
            pl.semaphore_wait(barrier, 1)

        @pl.when((core == 1) & jnp.logical_not(root))
        def _():
            pl.semaphore_wait(barrier, 1 + len(links))

        @pl.when(root)
        def _():
            pl.semaphore_wait(barrier, 1 + len(links) + n_section - 1)

        @pl.when(core == 1)
        def _():
            to_shards(heard.at[0], links)

    for p in range(PARTS0):
        wait_bytes(ahead.at[0, :, pl.ds(0, 4 * size0)], ahead_sem.at[p])
        for h, q in first4:
            pair0(p, h, q).start()
    small = [
        pltpu.make_async_copy(a, b, small_sem.at[k])
        for k, (a, b) in enumerate(((layer_hbm, layer), (valid_hbm, valid), (decay_hbm, decay)))
    ]
    io = [
        pltpu.make_async_copy(params, w_buf, io_sem.at[0]),
        pltpu.make_async_copy(m_first, f_buf, io_sem.at[1]),
        pltpu.make_async_copy(m_second, s_buf, io_sem.at[1]),
    ]
    for g in range(1, len(groups)):
        for h, block in groups[g]:
            pair(h, block).start()
        if g > 1:
            for h, block in groups[g]:
                load(h, block).start()
        if g == 4:
            for c in small + io:
                c.start()

    ready = {0}

    def need(h, block):
        g = group_of[h, block]
        if g not in ready:
            ready.add(g)
            wait_bytes(mine.at[0, pl.ds(0, 2 * len(groups[g]))], here_sem.at[g])

    signs = (1, 3)
    each = [(axis, d, 2 * axis + d) for axis in (0, 1) for d in (0, 1)]
    four, eight = landed.at[0, pl.ds(0, 4)], landed.at[0, pl.ds(0, 8)]

    def own_terms(axis, block, q):
        need(axis, block)
        return [quarter(mine, axis, block, q), quarter(theirs, axis, block, q)]

    def far_first():
        wait_bytes(mine.at[0, pl.ds(0, 2)], here_sem.at[0])
        for p in range(PARTS0):
            wait_bytes(ahead.at[0, :, pl.ds(0, 4 * size0)], start_recv.at[p])
            if p == 0:

                @pl.when(core == 0)
                def _():
                    pl.semaphore_wait(near_in, 1)

            for axis, d, link in each:
                here = pl.ds(p * size0, size0)
                terms = [t.at[:, here] for t in own_terms(axis, block_at(axis, 2, 2), d)]
                add_up(terms[0], terms)
                send(link, terms[0], landed.at[link, FAR[0], :, here], far_recv.at[0])
            if p == 0:
                hear(0)

    def far(j):
        for axis, d, link in each:
            terms = own_terms(axis, block_at(axis, 2, ORDER[j]), d)
            add_up(terms[0], terms)
            send(link, terms[0], landed.at[link, FAR[j]], far_recv.at[j])

    def near_own(j):
        for axis, d, link in each:
            terms = own_terms(axis, block_at(axis, signs[d], ORDER[j]), 1 - d)
            add_up(terms[0], terms)
            send(link, terms[0], landed.at[link, NEAR_OWN[j]], near_recv.at[j])

    def near_sum(j):
        wait_bytes(four, far_recv.at[j])
        for axis, d, link in each:
            terms = own_terms(axis, block_at(axis, signs[d], ORDER[j]), d)
            add_up(terms[0], terms + [landed.at[link, FAR[j]]])
            send(link, terms[0], landed.at[link, NEAR_SUM[j]], near_recv.at[j])

    def first_axis(axis, j):
        block = block_at(axis, 0, ORDER[j])
        a, b = 2 * axis, 2 * axis + 1
        return [
            own_terms(axis, block, q)
            + [landed.at[(a, b)[q], NEAR_SUM[j]], landed.at[(b, a)[q], NEAR_OWN[j]]]
            for q in (0, 1)
        ]

    def settle(j):
        wait_bytes(eight, near_recv.at[j])
        for axis in (0, 1):
            for terms in first_axis(axis, j):
                add_up(terms[0], terms)

    def far2():
        settle(0)
        for axis, d, _ in each:
            link = 2 * (1 - axis) + d
            send(link, quarter(mine, axis, block_at(axis, 0, 2), d), landed.at[link, FAR2], far2_recv)

    def own2():
        settle(1)
        settle(2)
        for axis, d, _ in each:
            link = 2 * (1 - axis) + d
            src = quarter(mine, axis, block_at(axis, 0, signs[d]), 1 - d)
            send(link, src, landed.at[link, OWN2], own2_recv, own2_send)

    def sum2():
        wait_bytes(four, far2_recv)

        for p, (start, size) in enumerate(parts):
            if p == 1:
                @pl.when(core == 1)
                def _():
                    pl.semaphore_wait(go_on, 1)

            for axis, d, _ in each:
                link = 2 * (1 - axis) + d
                at = pl.ds(start, size)
                dst = quarter(mine, axis, block_at(axis, 0, signs[d]), d).at[:, at]
                add_up(dst, [dst, landed.at[link, FAR2].at[:, at]])
                send(link, dst, late.at[link, :, at], sum2_recv.at[p], sum2_send)

    with jax.named_scope("far0"):
        far_first()
    for j in range(1, 4):
        with jax.named_scope(f"far{j}"):
            far(j)
        hear(j)
    for j in range(3):
        with jax.named_scope(f"own{j}"):
            near_own(j)
        with jax.named_scope(f"sum{j}"):
            near_sum(j)
        if j == 1:
            hear_roots()
    near_own(3)

    @pl.when(jnp.logical_not(root))
    def _():
        pl.semaphore_wait(all_in, 1)


    for c in small + io[:1]:
        c.wait()
    wait_bytes(theirs.at[0, pl.ds(0, 8)], io_sem.at[1])
    row_block = lax.broadcasted_iota(jnp.int32, (rows, 128), 0) // 8
    blocks = rows // 8

    def per_row(values):
        out = jnp.full((rows, 128), values[0])
        for b in range(1, blocks):
            out = jnp.where(row_block == b, values[b], out)
        return out

    layers = [layer[0, b] for b in range(blocks)]
    lives = [valid[0, b] for b in range(blocks)]
    row_decay = per_row([decay[l] for l in layers])
    row_live = per_row(lives) > 0

    row_layer = per_row(layers)
    row_lane = lax.broadcasted_iota(jnp.int32, (rows, 128), 1)
    own_lane = (row_lane == row_layer) & row_live
    own_lane_w = (row_lane == row_layer + 8) & row_live
    out_mask[...] = jnp.where(own_lane, 1.0, 0.0)

    def by_layer(total, lanes):
        in_row = jnp.sum(total, axis=1, keepdims=True)
        return jnp.sum(jnp.where(lanes, in_row, 0.0), axis=0, keepdims=True)

    piece = 512

    def weights_sq(i, acc):
        for k in range(piece // 128):
            v = w_buf[0, :, pl.ds(pl.multiple_of(i * piece + k * 128, 128), 128)].astype(F32)
            acc = acc + v * v
        return acc

    w_sum = by_layer(lax.fori_loop(0, columns // piece, weights_sq, jnp.zeros((rows, 128), F32)), own_lane_w)

    with jax.named_scope("far2"):
        far2()
    with jax.named_scope("near_sum3"):
        near_sum(3)
    with jax.named_scope("own2"):
        own2()
    with jax.named_scope("sum2"):
        sum2()

    with jax.named_scope("own2_sent"):
        wait_bytes(four, own2_send)

        @pl.when(core == 0)
        def _():
            to_shards(go_on, (partner,))

    with jax.named_scope("early"):
        wait_bytes(eight, near_recv.at[3])
        for axis in (0, 1):
            both = first_axis(axis, 3)
            if axis == 0:
                wait_bytes(four, own2_recv)
            for q in (0, 1):
                terms = both[q] + [landed.at[2 * (1 - axis) + 1 - q, OWN2]]
                base = (2 * axis + q) * width

                def before(i, _, terms=terms, base=base):
                    at = pl.multiple_of(i * min(512, width), min(512, width))
                    here = pl.ds(at, min(512, width))
                    g = terms[0][:, here].astype(F32)
                    for t in terms[1:]:
                        g = g + t[:, here].astype(F32)
                    upd[0, :, pl.ds(base + at, min(512, width))] = g
                    return 0

                lax.fori_loop(0, width // min(512, width), before, 0)

    acc = jnp.zeros((rows, 128), F32)
    for p, (start, part) in enumerate(parts):
        with jax.named_scope(f"late{p}"):
            wait_bytes(late.at[:, :, pl.ds(start, part)], sum2_recv.at[p])
        for axis in (0, 1):
            for q in (0, 1):
                came = late.at[2 * (1 - axis) + q, :, pl.ds(start, part)]
                base = (2 * axis + q) * width + start
                step = min(512, part)
                assert part % step == 0

                def one(i, acc, came=came, base=base, step=step):
                    for k in range(step // 128):
                        at = i * step + k * 128
                        cols = pl.ds(pl.multiple_of(base + at, 128), 128)
                        g = upd[0, :, cols] + came[:, pl.ds(pl.multiple_of(at, 128), 128)].astype(F32)
                        old_f, old_s = f_buf[0, :, cols], s_buf[0, :, cols]
                        w = w_buf[0, :, cols].astype(F32)
                        first = 0.9 * old_f + 0.1 * g
                        second = 0.99 * old_s + 0.01 * g * g
                        u = (first * (1.0 / bias_first)) / (
                            jnp.sqrt(second * (1.0 / bias_second)) + 1e-06
                        ) + row_decay * w
                        upd[0, :, cols] = u
                        f_buf[0, :, cols] = jnp.where(row_live, first, old_f)
                        s_buf[0, :, cols] = jnp.where(row_live, second, old_s)
                        acc = acc + u * u
                    return acc

                acc = lax.fori_loop(0, part // step, one, acc)

    vec = by_layer(acc, own_lane) + w_sum
    sums[0] = vec
    got[me] = vec

    def tell(to_section, to_shard):
        pltpu.make_async_remote_copy(
            src_ref=sums.at[0],
            dst_ref=got.at[me],
            send_sem=sum_send,
            recv_sem=sum_recv,
            device_id={"section": to_section, "shard": to_shard},
            device_id_type=MESH,
        ).start()

    far_from = (0, 1, 2, 1)
    away = sorted(
        ((ds, dy, dx, c) for ds in range(n_section) for dy in range(SIDE) for dx in range(SIDE) for c in (0, 1)),
        key=lambda a: -sum(far_from[k] for k in a[:3]) - a[3] / 2,
    )
    sections = [lax.rem(section + k, n_section) for k in range(n_section)]
    shards_at = {
        (dy, dx, c): chip_at(dy, dx) * 2 + (core if c == 0 else 1 - core)
        for dy in range(SIDE) for dx in range(SIDE) for c in (0, 1)
    }
    with jax.named_scope("tell"):
        for ds, dy, dx, c in away[:-1]:
            tell(sections[ds], shards_at[dy, dx, c])
    n_all = n_section * n_shard
    others = got.at[pl.ds(0, n_all - 1)]
    with jax.named_scope("everyone"):
        wait_bytes(others, sum_recv)

    with jax.named_scope("drain"):
        wait_bytes(theirs, pair_send)
        wait_bytes(landed.at[:, pl.ds(0, SLOTS - 1)], link_send)
        wait_bytes(late, sum2_send)
        wait_bytes(others, sum_send)


def finish(upd, first, second, weights, mask, got, out_params, out_first, out_second, out_ratios, stage, ratio, sem):
    columns = stage.shape[1]
    step = columns // 4
    copies = [
        pltpu.make_async_copy(first, out_first, sem.at[0]),
        pltpu.make_async_copy(second, out_second, sem.at[1]),
    ]
    for c in copies:
        c.start()
    several = [got[k] for k in range(8)]
    for k in range(8, got.shape[0]):
        several[k % 8] = several[k % 8] + got[k]
    while len(several) > 1:
        several = [a + b for a, b in zip(several[::2], several[1::2])]
    wide = jnp.broadcast_to(several[0], (8, 128))
    lane = lax.broadcasted_iota(jnp.int32, (1, 128), 1)
    ratios = jnp.sqrt(pltpu.roll(wide, 120, 1) / (wide + 1.0))[0:1]
    ratios = jnp.where(lane < ratio.shape[1], ratios, 0.0)
    ratio[...] = ratios[:, : ratio.shape[1]]
    c = pltpu.make_async_copy(ratio, out_ratios, sem.at[6])
    c.start()
    copies.append(c)
    row_ratio = jnp.sum(jnp.where(mask[...] > 0.5, ratios, 0.0), axis=1, keepdims=True)
    row_scale = jnp.broadcast_to(0.1 * row_ratio, mask.shape)
    for n in range(4):
      with jax.named_scope(f"fin{n}"):

        def one(i, _, n=n):
            for k in range(4):
                cols = pl.ds(pl.multiple_of(n * step + i * 512 + k * 128, 128), 128)
                w = weights[0, :, cols].astype(F32)
                stage[:, cols] = (w - row_scale * upd[0, :, cols]).astype(BF16)
            return 0

        lax.fori_loop(0, step // 512, one, 0)
        cols = pl.ds(n * step, step)
        c = pltpu.make_async_copy(stage.at[:, cols], out_params.at[0, :, cols], sem.at[2 + n])
        c.start()
        copies.append(c)
    with jax.named_scope("finw"):
      for c in copies:
        c.wait()


PARTS = (4, 4, 4, 2, 2)
PARTS0 = 4
ROUNDS = 4


def shards(grad_parts, params, moment_first, moment_second, block_layer, block_valid, decay):
    rows, columns = params.shape[1:]
    n_section, n_shard = lax.axis_size("section"), lax.axis_size("shard")
    width = columns // 4
    chips = SIDE * SIDE
    hbm, vmem = pl.BlockSpec(memory_space=pltpu.HBM), pl.BlockSpec(memory_space=pltpu.VMEM)
    dma = pltpu.SemaphoreType.DMA
    groups = 8
    upd, first, second, weights, mask, got = pl.pallas_call(
        functools.partial(kernel, n_section, n_shard),
        out_shape=(
            pltpu.VMEM(moment_first.shape, F32),
            pltpu.VMEM(moment_first.shape, F32),
            pltpu.VMEM(moment_first.shape, F32),
            pltpu.VMEM(params.shape, BF16),
            pltpu.VMEM((rows, 128), F32),
            pltpu.VMEM((n_section * n_shard, 1, 128), F32),
        ),
        in_specs=[hbm] * 7,
        out_specs=(vmem,) * 6,
        scratch_shapes=[
            pltpu.VMEM((2, chips, rows, 2 * width), BF16),
            pltpu.VMEM((2, chips, rows, 2 * width), BF16),
            pltpu.VMEM((2, rows, 2 * width), BF16),
            pltpu.VMEM((4, SLOTS, rows, width), BF16),
            pltpu.VMEM((4, rows, width), BF16),
            pltpu.SMEM(block_layer.shape, jnp.int32),
            pltpu.SMEM(block_valid.shape, jnp.int32),
            pltpu.SMEM(decay.shape, F32),
            pltpu.VMEM((1, 1, 128), F32),
            dma((groups,)),
            dma,
            dma,
            dma((4,)),
            dma((4,)),
            dma,
            dma,
            dma,
            dma((len(PARTS),)),
            dma,
            dma((PARTS0,)),
            pltpu.SemaphoreType.REGULAR((ROUNDS,)),
            pltpu.SemaphoreType.REGULAR,
            pltpu.SemaphoreType.REGULAR,
            pltpu.SemaphoreType.REGULAR,
            pltpu.SemaphoreType.REGULAR,
            dma((PARTS0,)),
            dma((3,)),
            dma((2,)),
            dma,
            dma,
        ],
        compiler_params=pltpu.CompilerParams(
            collective_id=0, has_side_effects=True, vmem_limit_bytes=48 * 2**20
        ),
        name="lamb_step",
    )(*(
        pltpu.with_memory_space_constraint(a, pltpu.HBM)
        for a in (grad_parts, params, moment_first, moment_second, block_layer, block_valid, decay)
    ))
    new_params, new_first, new_second, ratios = pl.pallas_call(
        finish,
        out_shape=(
            jax.ShapeDtypeStruct(params.shape, params.dtype),
            jax.ShapeDtypeStruct(moment_first.shape, F32),
            jax.ShapeDtypeStruct(moment_second.shape, F32),
            jax.ShapeDtypeStruct((1, decay.shape[0]), F32),
        ),
        in_specs=[vmem] * 6,
        out_specs=(hbm,) * 4,
        scratch_shapes=[pltpu.VMEM((rows, columns), BF16), pltpu.VMEM((1, decay.shape[0]), F32), dma((7,))],
        compiler_params=pltpu.CompilerParams(vmem_limit_bytes=8 * 2**20),
        name="finish",
    )(upd, first, second, weights, mask, got)
    return new_params, new_first, new_second, ratios[0]


def solution(mesh):
    placed = (
        P("section", "shard", None, None),
        P("section", "shard", None),
        P("section", "shard", None),
        P("section", "shard", None),
        P("section", "shard"),
        P("section", "shard"),
        P(),
    )
    return jax.shard_map(
        shards,
        mesh=mesh,
        in_specs=placed,
        out_specs=(
            P("section", "shard", None),
            P("section", "shard", None),
            P("section", "shard", None),
            P(),
        ),
        check_vma=False,
    )
```

```python
import functools

import jax
import jax.numpy as jnp
from jax import lax
from jax.experimental import pallas as pl
from jax.experimental.pallas import tpu as pltpu
from jax.sharding import PartitionSpec as P

bias_first = 1.0 - 0.9**10
bias_second = 1.0 - 0.99**10

MESH = pl.DeviceIdType.MESH
F32, BF16 = jnp.float32, jnp.bfloat16
SIDE = 4
ORDER = (2, 1, 3, 0)
FAR, NEAR_OWN, NEAR_SUM = (0, 1, 2, 3), (4, 6, 8, 10), (5, 7, 9, 11)
FAR2, OWN2 = 12, 13
SLOTS = 14


def block_at(axis, main, other):
    return other * SIDE + main if axis == 0 else main * SIDE + other


def kernel(
    n_section, n_shard,
    grads, params, m_first, m_second, layer_hbm, valid_hbm, decay_hbm,
    upd, f_buf, s_buf, w_buf, out_mask, got,
    mine, theirs, landed, late, layer, valid, decay, sums,
    here_sem, pair_send, link_send, far_recv, near_recv, far2_recv, own2_recv, own2_send, sum2_recv, sum2_send,
    start_recv, heard, near_in, roots_in, all_in, go_on, small_sem, io_sem, sum_send, sum_recv,
):
    rows = w_buf.shape[1]
    columns = w_buf.shape[2]
    width = landed.shape[3]
    parts = [(sum(PARTS[:p]) * (width // 16), PARTS[p] * (width // 16)) for p in range(len(PARTS))]
    section, shard = lax.axis_index("section"), lax.axis_index("shard")
    core, x, y = lax.rem(shard, 2), lax.rem(lax.div(shard, 2), SIDE), lax.div(shard, 2 * SIDE)
    me = section * n_shard + shard
    partner = shard + 1 - 2 * core

    def chip_at(dy, dx):
        return lax.rem(y + dy, SIDE) * SIDE + lax.rem(x + dx, SIDE)

    links = tuple(chip_at(dy, dx) * 2 + core for dy, dx in ((0, 1), (0, 3), (1, 0), (3, 0)))

    root = (core == 1) & (x == 0) & (y == 0)

    def to_shards(sem, peers):
        for peer in peers:
            pl.semaphore_signal(sem, inc=1, device_id={"shard": peer}, device_id_type=MESH)

    def to_roots(sem):
        for k in range(1, n_section):
            pl.semaphore_signal(
                sem, inc=1, device_id={"section": lax.rem(section + k, n_section)}, device_id_type=MESH
            )

    barrier = pltpu.get_barrier_semaphore()
    to_shards(barrier, (partner,))

    @pl.when(core == 1)
    def _():
        to_shards(barrier, links)

    @pl.when(root)
    def _():
        to_roots(barrier)

    def hear(k):
        @pl.when(core == 1)
        def _():
            pl.semaphore_wait(heard.at[k], len(links))
            if k + 1 < ROUNDS:
                to_shards(heard.at[k + 1], links)
            if k == 0:
                to_shards(near_in, (partner,))

        if k + 1 == ROUNDS:

            @pl.when(root)
            def _():
                to_roots(roots_in)

    def hear_roots():
        @pl.when(root)
        def _():
            pl.semaphore_wait(roots_in, n_section - 1)
            to_shards(all_in, [k for k in range(n_shard) if k != 1])

    groups = []
    for j in ORDER:
        groups.append([(h, block_at(h, 2, j)) for h in (0, 1)])
    for j in ORDER:
        groups.append([(h, block_at(h, main, j)) for main in (1, 3, 0) for h in (0, 1)])
    group_of = {b: g for g, blocks in enumerate(groups) for b in blocks}

    size0 = width // PARTS0
    first4 = [(h, q) for h in (0, 1) for q in (0, 1)]

    def source(h, block, which):
        chip = chip_at(block // SIDE, block % SIDE)
        at = pl.multiple_of(chip * (2 * rows) + which * rows, rows)
        return grads.at[0, 0, pl.ds(at, rows), pl.ds(h * 2 * width, 2 * width)]

    def load(h, block):
        return pltpu.make_async_copy(
            source(h, block, core), mine.at[h, block], here_sem.at[group_of[h, block]]
        )

    def load(h, block):
        return pltpu.make_async_copy(
            source(h, block, core), mine.at[h, block], here_sem.at[group_of[h, block]]
        )

    def fetch_ahead(p, h, q):
        cols = pl.ds(q * width + p * size0, size0)
        return pltpu.make_async_copy(
            source(h, block_at(h, 2, 2), 1 - core).at[:, cols], ahead.at[h, :, cols], ahead_sem.at[p]
        )

    def pair(h, block):
        return pltpu.make_async_remote_copy(
            src_ref=source(h, block, 1 - core),
            dst_ref=theirs.at[h, block],
            send_sem=pair_send,
            recv_sem=here_sem.at[group_of[h, block]],
            device_id={"shard": partner},
            device_id_type=MESH,
        )

    def pair0(p, h, q):
        cols = pl.ds(q * width + p * size0, size0)
        return pltpu.make_async_remote_copy(
            src_ref=source(h, block_at(h, 2, 2), 1 - core).at[:, cols],
            dst_ref=theirs.at[h, block_at(h, 2, 2), :, cols],
            send_sem=pair_send,
            recv_sem=start_recv.at[p],
            device_id={"shard": partner},
            device_id_type=MESH,
        )

    def wait_bytes(ref, sem):
        pltpu.make_async_copy(ref, ref, sem).wait()

    def quarter(ref, h, block, q):
        return ref.at[h, block, :, pl.ds(q * width, width)]

    def send(link, src, dst, recv_sem, send_sem=link_send):
        pltpu.make_async_remote_copy(
            src_ref=src,
            dst_ref=dst,
            send_sem=send_sem,
            recv_sem=recv_sem,
            device_id={"shard": links[link]},
            device_id_type=MESH,
        ).start()

    def add_up(dst, terms):
        size = dst.shape[1]
        step = min(512, size)
        assert size % step == 0

        def one(i, _):
            cols = pl.ds(pl.multiple_of(i * step, step), step)
            if len(terms) == 2:
                dst[:, cols] = terms[0][:, cols] + terms[1][:, cols]
            else:
                total = terms[0][:, cols].astype(F32)
                for t in terms[1:]:
                    total = total + t[:, cols].astype(F32)
                dst[:, cols] = total.astype(BF16)
            return 0

        lax.fori_loop(0, size // step, one, 0)

    for h, block in groups[0] + groups[1]:
        load(h, block).start()
    with jax.named_scope("barrier"):
        @pl.when(core == 0)
        def _():
            pl.semaphore_wait(barrier, 1)

        @pl.when((core == 1) & jnp.logical_not(root))
        def _():
            pl.semaphore_wait(barrier, 1 + len(links))

        @pl.when(root)
        def _():
            pl.semaphore_wait(barrier, 1 + len(links) + n_section - 1)

        @pl.when(core == 1)
        def _():
            to_shards(heard.at[0], links)

    for p in range(PARTS0):
        for h, q in first4:
            pair0(p, h, q).start()
    small = [
        pltpu.make_async_copy(a, b, small_sem.at[k])
        for k, (a, b) in enumerate(((layer_hbm, layer), (valid_hbm, valid), (decay_hbm, decay)))
    ]
    io = [
        pltpu.make_async_copy(params, w_buf, io_sem.at[0]),
        pltpu.make_async_copy(m_first, f_buf, io_sem.at[1]),
        pltpu.make_async_copy(m_second, s_buf, io_sem.at[1]),
    ]
    for g in range(1, len(groups)):
        for h, block in groups[g]:
            pair(h, block).start()
        if g > 1:
            for h, block in groups[g]:
                load(h, block).start()
        if g == 4:
            for c in small + io:
                c.start()

    ready = {0}

    def need(h, block):
        g = group_of[h, block]
        if g not in ready:
            ready.add(g)
            wait_bytes(mine.at[0, pl.ds(0, 2 * len(groups[g]))], here_sem.at[g])

    signs = (1, 3)
    each = [(axis, d, 2 * axis + d) for axis in (0, 1) for d in (0, 1)]
    four, eight = landed.at[0, pl.ds(0, 4)], landed.at[0, pl.ds(0, 8)]

    def own_terms(axis, block, q):
        need(axis, block)
        return [quarter(mine, axis, block, q), quarter(theirs, axis, block, q)]

    def far_first():
        wait_bytes(mine.at[0, pl.ds(0, 2)], here_sem.at[0])
        for p in range(PARTS0):
            wait_bytes(landed.at[0, 0, :, pl.ds(0, 4 * size0)], start_recv.at[p])
            if p == 0:

                @pl.when(core == 0)
                def _():
                    pl.semaphore_wait(near_in, 1)

            for axis, d, link in each:
                here = pl.ds(p * size0, size0)
                terms = [t.at[:, here] for t in own_terms(axis, block_at(axis, 2, 2), d)]
                add_up(terms[0], terms)
                send(link, terms[0], landed.at[link, FAR[0], :, here], far_recv.at[0])
        hear(0)

    def far(j):
        for axis, d, link in each:
            terms = own_terms(axis, block_at(axis, 2, ORDER[j]), d)
            add_up(terms[0], terms)
            send(link, terms[0], landed.at[link, FAR[j]], far_recv.at[j])

    def near_own(j):
        for axis, d, link in each:
            terms = own_terms(axis, block_at(axis, signs[d], ORDER[j]), 1 - d)
            add_up(terms[0], terms)
            send(link, terms[0], landed.at[link, NEAR_OWN[j]], near_recv.at[j])

    def near_sum(j):
        wait_bytes(four, far_recv.at[j])
        for axis, d, link in each:
            terms = own_terms(axis, block_at(axis, signs[d], ORDER[j]), d)
            add_up(terms[0], terms + [landed.at[link, FAR[j]]])
            send(link, terms[0], landed.at[link, NEAR_SUM[j]], near_recv.at[j])

    def first_axis(axis, j):
        block = block_at(axis, 0, ORDER[j])
        a, b = 2 * axis, 2 * axis + 1
        return [
            own_terms(axis, block, q)
            + [landed.at[(a, b)[q], NEAR_SUM[j]], landed.at[(b, a)[q], NEAR_OWN[j]]]
            for q in (0, 1)
        ]

    def settle(j):
        wait_bytes(eight, near_recv.at[j])
        for axis in (0, 1):
            for terms in first_axis(axis, j):
                add_up(terms[0], terms)

    def far2():
        settle(0)
        for axis, d, _ in each:
            link = 2 * (1 - axis) + d
            send(link, quarter(mine, axis, block_at(axis, 0, 2), d), landed.at[link, FAR2], far2_recv)

    def own2():
        settle(1)
        settle(2)
        for axis, d, _ in each:
            link = 2 * (1 - axis) + d
            src = quarter(mine, axis, block_at(axis, 0, signs[d]), 1 - d)
            send(link, src, landed.at[link, OWN2], own2_recv, own2_send)

    def sum2():
        wait_bytes(four, far2_recv)

        for p, (start, size) in enumerate(parts):
            if p == 0:
                @pl.when(core == 1)
                def _():
                    pl.semaphore_wait(go_on, 1)

            for axis, d, _ in each:
                link = 2 * (1 - axis) + d
                at = pl.ds(start, size)
                dst = quarter(mine, axis, block_at(axis, 0, signs[d]), d).at[:, at]
                add_up(dst, [dst, landed.at[link, FAR2].at[:, at]])
                send(link, dst, late.at[link, :, at], sum2_recv.at[p], sum2_send)

    with jax.named_scope("far0"):
        far_first()
    for j in range(1, 4):
        with jax.named_scope(f"far{j}"):
            far(j)
        hear(j)
    for j in range(3):
        with jax.named_scope(f"own{j}"):
            near_own(j)
        with jax.named_scope(f"sum{j}"):
            near_sum(j)
        if j == 1:
            hear_roots()
    near_own(3)

    @pl.when(jnp.logical_not(root))
    def _():
        pl.semaphore_wait(all_in, 1)


    for c in small + io[:1]:
        c.wait()
    wait_bytes(theirs.at[0, pl.ds(0, 8)], io_sem.at[1])
    row_block = lax.broadcasted_iota(jnp.int32, (rows, 128), 0) // 8
    blocks = rows // 8

    def per_row(values):
        out = jnp.full((rows, 128), values[0])
        for b in range(1, blocks):
            out = jnp.where(row_block == b, values[b], out)
        return out

    layers = [layer[0, b] for b in range(blocks)]
    lives = [valid[0, b] for b in range(blocks)]
    row_decay = per_row([decay[l] for l in layers])
    row_live = per_row(lives) > 0

    row_layer = per_row(layers)
    row_lane = lax.broadcasted_iota(jnp.int32, (rows, 128), 1)
    own_lane = (row_lane == row_layer) & row_live
    own_lane_w = (row_lane == row_layer + 8) & row_live
    out_mask[...] = jnp.where(own_lane, 1.0, 0.0)

    def by_layer(total, lanes):
        in_row = jnp.sum(total, axis=1, keepdims=True)
        return jnp.sum(jnp.where(lanes, in_row, 0.0), axis=0, keepdims=True)

    piece = 512

    def weights_sq(i, acc):
        for k in range(piece // 128):
            v = w_buf[0, :, pl.ds(pl.multiple_of(i * piece + k * 128, 128), 128)].astype(F32)
            acc = acc + v * v
        return acc

    w_sum = by_layer(lax.fori_loop(0, columns // piece, weights_sq, jnp.zeros((rows, 128), F32)), own_lane_w)

    with jax.named_scope("far2"):
        far2()
    with jax.named_scope("near_sum3"):
        near_sum(3)
    with jax.named_scope("own2"):
        own2()
    with jax.named_scope("sum2"):
        sum2()

    with jax.named_scope("own2_sent"):
        wait_bytes(four, own2_send)

        @pl.when(core == 0)
        def _():
            to_shards(go_on, (partner,))

    with jax.named_scope("early"):
        wait_bytes(eight, near_recv.at[3])
        for axis in (0, 1):
            both = first_axis(axis, 3)
            if axis == 0:
                wait_bytes(four, own2_recv)
            for q in (0, 1):
                terms = both[q] + [landed.at[2 * (1 - axis) + 1 - q, OWN2]]
                base = (2 * axis + q) * width

                def before(i, _, terms=terms, base=base):
                    at = pl.multiple_of(i * min(512, width), min(512, width))
                    here = pl.ds(at, min(512, width))
                    g = terms[0][:, here].astype(F32)
                    for t in terms[1:]:
                        g = g + t[:, here].astype(F32)
                    upd[0, :, pl.ds(base + at, min(512, width))] = g
                    return 0

                lax.fori_loop(0, width // min(512, width), before, 0)

    acc = jnp.zeros((rows, 128), F32)
    for p, (start, part) in enumerate(parts):
        with jax.named_scope(f"late{p}"):
            wait_bytes(late.at[:, :, pl.ds(start, part)], sum2_recv.at[p])
        for axis in (0, 1):
            for q in (0, 1):
                came = late.at[2 * (1 - axis) + q, :, pl.ds(start, part)]
                base = (2 * axis + q) * width + start
                step = min(512, part)
                assert part % step == 0

                def one(i, acc, came=came, base=base, step=step):
                    for k in range(step // 128):
                        at = i * step + k * 128
                        cols = pl.ds(pl.multiple_of(base + at, 128), 128)
                        g = upd[0, :, cols] + came[:, pl.ds(pl.multiple_of(at, 128), 128)].astype(F32)
                        old_f, old_s = f_buf[0, :, cols], s_buf[0, :, cols]
                        w = w_buf[0, :, cols].astype(F32)
                        first = 0.9 * old_f + 0.1 * g
                        second = 0.99 * old_s + 0.01 * g * g
                        u = (first * (1.0 / bias_first)) / (
                            jnp.sqrt(second * (1.0 / bias_second)) + 1e-06
                        ) + row_decay * w
                        upd[0, :, cols] = u
                        f_buf[0, :, cols] = jnp.where(row_live, first, old_f)
                        s_buf[0, :, cols] = jnp.where(row_live, second, old_s)
                        acc = acc + u * u
                    return acc

                acc = lax.fori_loop(0, part // step, one, acc)

    vec = by_layer(acc, own_lane) + w_sum
    sums[0] = vec
    got[me] = vec

    def tell(to_section, to_shard):
        pltpu.make_async_remote_copy(
            src_ref=sums.at[0],
            dst_ref=got.at[me],
            send_sem=sum_send,
            recv_sem=sum_recv,
            device_id={"section": to_section, "shard": to_shard},
            device_id_type=MESH,
        ).start()

    far_from = (0, 1, 2, 1)
    away = sorted(
        ((ds, dy, dx, c) for ds in range(n_section) for dy in range(SIDE) for dx in range(SIDE) for c in (0, 1)),
        key=lambda a: -sum(far_from[k] for k in a[:3]) - a[3] / 2,
    )
    sections = [lax.rem(section + k, n_section) for k in range(n_section)]
    shards_at = {
        (dy, dx, c): chip_at(dy, dx) * 2 + (core if c == 0 else 1 - core)
        for dy in range(SIDE) for dx in range(SIDE) for c in (0, 1)
    }
    with jax.named_scope("tell"):
        for ds, dy, dx, c in away[:-1]:
            tell(sections[ds], shards_at[dy, dx, c])
    n_all = n_section * n_shard
    others = got.at[pl.ds(0, n_all - 1)]
    with jax.named_scope("everyone"):
        wait_bytes(others, sum_recv)

    with jax.named_scope("drain"):
        wait_bytes(theirs, pair_send)
        wait_bytes(landed.at[:, pl.ds(0, SLOTS - 1)], link_send)
        wait_bytes(late, sum2_send)
        wait_bytes(others, sum_send)


def finish(upd, first, second, weights, mask, got, out_params, out_first, out_second, out_ratios, stage, ratio, sem):
    columns = stage.shape[1]
    step = columns // 4
    copies = [
        pltpu.make_async_copy(first, out_first, sem.at[0]),
        pltpu.make_async_copy(second, out_second, sem.at[1]),
    ]
    for c in copies:
        c.start()
    several = [got[k] for k in range(8)]
    for k in range(8, got.shape[0]):
        several[k % 8] = several[k % 8] + got[k]
    while len(several) > 1:
        several = [a + b for a, b in zip(several[::2], several[1::2])]
    wide = jnp.broadcast_to(several[0], (8, 128))
    lane = lax.broadcasted_iota(jnp.int32, (1, 128), 1)
    ratios = jnp.sqrt(pltpu.roll(wide, 120, 1) / (wide + 1.0))[0:1]
    ratios = jnp.where(lane < ratio.shape[1], ratios, 0.0)
    ratio[...] = ratios[:, : ratio.shape[1]]
    c = pltpu.make_async_copy(ratio, out_ratios, sem.at[6])
    c.start()
    copies.append(c)
    row_ratio = jnp.sum(jnp.where(mask[...] > 0.5, ratios, 0.0), axis=1, keepdims=True)
    row_scale = jnp.broadcast_to(0.1 * row_ratio, mask.shape)
    for n in range(4):
      with jax.named_scope(f"fin{n}"):

        def one(i, _, n=n):
            for k in range(4):
                cols = pl.ds(pl.multiple_of(n * step + i * 512 + k * 128, 128), 128)
                w = weights[0, :, cols].astype(F32)
                stage[:, cols] = (w - row_scale * upd[0, :, cols]).astype(BF16)
            return 0

        lax.fori_loop(0, step // 512, one, 0)
        cols = pl.ds(n * step, step)
        c = pltpu.make_async_copy(stage.at[:, cols], out_params.at[0, :, cols], sem.at[2 + n])
        c.start()
        copies.append(c)
    with jax.named_scope("finw"):
      for c in copies:
        c.wait()


PARTS = (4, 4, 4, 2, 2)
PARTS0 = 4
ROUNDS = 4


def shards(grad_parts, params, moment_first, moment_second, block_layer, block_valid, decay):
    rows, columns = params.shape[1:]
    n_section, n_shard = lax.axis_size("section"), lax.axis_size("shard")
    width = columns // 4
    chips = SIDE * SIDE
    hbm, vmem = pl.BlockSpec(memory_space=pltpu.HBM), pl.BlockSpec(memory_space=pltpu.VMEM)
    dma = pltpu.SemaphoreType.DMA
    groups = 8
    upd, first, second, weights, mask, got = pl.pallas_call(
        functools.partial(kernel, n_section, n_shard),
        out_shape=(
            pltpu.VMEM(moment_first.shape, F32),
            pltpu.VMEM(moment_first.shape, F32),
            pltpu.VMEM(moment_first.shape, F32),
            pltpu.VMEM(params.shape, BF16),
            pltpu.VMEM((rows, 128), F32),
            pltpu.VMEM((n_section * n_shard, 1, 128), F32),
        ),
        in_specs=[hbm] * 7,
        out_specs=(vmem,) * 6,
        scratch_shapes=[
            pltpu.VMEM((2, chips, rows, 2 * width), BF16),
            pltpu.VMEM((2, chips, rows, 2 * width), BF16),
            pltpu.VMEM((4, SLOTS, rows, width), BF16),
            pltpu.VMEM((4, rows, width), BF16),
            pltpu.SMEM(block_layer.shape, jnp.int32),
            pltpu.SMEM(block_valid.shape, jnp.int32),
            pltpu.SMEM(decay.shape, F32),
            pltpu.VMEM((1, 1, 128), F32),
            dma((groups,)),
            dma,
            dma,
            dma((4,)),
            dma((4,)),
            dma,
            dma,
            dma,
            dma((len(PARTS),)),
            dma,
            dma((PARTS0,)),
            pltpu.SemaphoreType.REGULAR((ROUNDS,)),
            pltpu.SemaphoreType.REGULAR,
            pltpu.SemaphoreType.REGULAR,
            pltpu.SemaphoreType.REGULAR,
            pltpu.SemaphoreType.REGULAR,
            dma((3,)),
            dma((2,)),
            dma,
            dma,
        ],
        compiler_params=pltpu.CompilerParams(
            collective_id=0, has_side_effects=True, vmem_limit_bytes=48 * 2**20
        ),
        name="lamb_step",
    )(*(
        pltpu.with_memory_space_constraint(a, pltpu.HBM)
        for a in (grad_parts, params, moment_first, moment_second, block_layer, block_valid, decay)
    ))
    new_params, new_first, new_second, ratios = pl.pallas_call(
        finish,
        out_shape=(
            jax.ShapeDtypeStruct(params.shape, params.dtype),
            jax.ShapeDtypeStruct(moment_first.shape, F32),
            jax.ShapeDtypeStruct(moment_second.shape, F32),
            jax.ShapeDtypeStruct((1, decay.shape[0]), F32),
        ),
        in_specs=[vmem] * 6,
        out_specs=(hbm,) * 4,
        scratch_shapes=[pltpu.VMEM((rows, columns), BF16), pltpu.VMEM((1, decay.shape[0]), F32), dma((7,))],
        compiler_params=pltpu.CompilerParams(vmem_limit_bytes=8 * 2**20),
        name="finish",
    )(upd, first, second, weights, mask, got)
    return new_params, new_first, new_second, ratios[0]


def solution(mesh):
    placed = (
        P("section", "shard", None, None),
        P("section", "shard", None),
        P("section", "shard", None),
        P("section", "shard", None),
        P("section", "shard"),
        P("section", "shard"),
        P(),
    )
    return jax.shard_map(
        shards,
        mesh=mesh,
        in_specs=placed,
        out_specs=(
            P("section", "shard", None),
            P("section", "shard", None),
            P("section", "shard", None),
            P(),
        ),
        check_vma=False,
    )
```

```python
import functools

import jax
import jax.numpy as jnp
from jax import lax
from jax.experimental import pallas as pl
from jax.experimental.pallas import tpu as pltpu
from jax.sharding import PartitionSpec as P

bias_first = 1.0 - 0.9**10
bias_second = 1.0 - 0.99**10

MESH = pl.DeviceIdType.MESH
F32, BF16 = jnp.float32, jnp.bfloat16
SIDE = 4
ORDER = (2, 1, 3, 0)
FAR, NEAR_OWN, NEAR_SUM = (0, 1, 2, 3), (4, 6, 8, 10), (5, 7, 9, 11)
FAR2, OWN2 = 12, 13
SLOTS = 14


def block_at(axis, main, other):
    return other * SIDE + main if axis == 0 else main * SIDE + other


def kernel(
    n_section, n_shard,
    grads, params, m_first, m_second, layer_hbm, valid_hbm, decay_hbm,
    upd, f_buf, s_buf, w_buf, out_mask, got,
    mine, theirs, landed, late, layer, valid, decay, sums,
    here_sem, pair_send, link_send, far_recv, near_recv, far2_recv, own2_recv, own2_send, sum2_recv, sum2_send,
    start_recv, heard, near_in, roots_in, all_in, go_on, small_sem, io_sem, sum_send, sum_recv,
):
    rows = w_buf.shape[1]
    columns = w_buf.shape[2]
    width = landed.shape[3]
    parts = [(sum(PARTS[:p]) * (width // 16), PARTS[p] * (width // 16)) for p in range(len(PARTS))]
    section, shard = lax.axis_index("section"), lax.axis_index("shard")
    core, x, y = lax.rem(shard, 2), lax.rem(lax.div(shard, 2), SIDE), lax.div(shard, 2 * SIDE)
    me = section * n_shard + shard
    partner = shard + 1 - 2 * core

    def chip_at(dy, dx):
        return lax.rem(y + dy, SIDE) * SIDE + lax.rem(x + dx, SIDE)

    links = tuple(chip_at(dy, dx) * 2 + core for dy, dx in ((0, 1), (0, 3), (1, 0), (3, 0)))

    root = (core == 1) & (x == 0) & (y == 0)

    def to_shards(sem, peers):
        for peer in peers:
            pl.semaphore_signal(sem, inc=1, device_id={"shard": peer}, device_id_type=MESH)

    def to_roots(sem):
        for k in range(1, n_section):
            pl.semaphore_signal(
                sem, inc=1, device_id={"section": lax.rem(section + k, n_section)}, device_id_type=MESH
            )

    barrier = pltpu.get_barrier_semaphore()
    to_shards(barrier, (partner,))

    @pl.when(core == 1)
    def _():
        to_shards(barrier, links)

    @pl.when(root)
    def _():
        to_roots(barrier)

    def hear(k):
        @pl.when(core == 1)
        def _():
            pl.semaphore_wait(heard.at[k], len(links))
            if k + 1 < ROUNDS:
                to_shards(heard.at[k + 1], links)
            if k == 0:
                to_shards(near_in, (partner,))

        if k + 1 == ROUNDS:

            @pl.when(root)
            def _():
                to_roots(roots_in)

    def hear_roots():
        @pl.when(root)
        def _():
            pl.semaphore_wait(roots_in, n_section - 1)
            to_shards(all_in, [k for k in range(n_shard) if k != 1])

    groups = []
    for j in ORDER:
        groups.append([(h, block_at(h, 2, j)) for h in (0, 1)])
    for some in (ORDER[:1], ORDER[1:2], ORDER[2:]):
        groups.append([(h, block_at(h, main, j)) for j in some for main in (1, 3, 0) for h in (0, 1)])
    group_of = {b: g for g, blocks in enumerate(groups) for b in blocks}

    size0 = width // PARTS0
    first4 = [(h, q) for h in (0, 1) for q in (0, 1)]

    def source(h, block, which):
        chip = chip_at(block // SIDE, block % SIDE)
        at = pl.multiple_of(chip * (2 * rows) + which * rows, rows)
        return grads.at[0, 0, pl.ds(at, rows), pl.ds(h * 2 * width, 2 * width)]

    def load(h, block):
        return pltpu.make_async_copy(
            source(h, block, core), mine.at[h, block], here_sem.at[group_of[h, block]]
        )

    def load(h, block):
        return pltpu.make_async_copy(
            source(h, block, core), mine.at[h, block], here_sem.at[group_of[h, block]]
        )

    def fetch_ahead(p, h, q):
        cols = pl.ds(q * width + p * size0, size0)
        return pltpu.make_async_copy(
            source(h, block_at(h, 2, 2), 1 - core).at[:, cols], ahead.at[h, :, cols], ahead_sem.at[p]
        )

    def pair(h, block):
        return pltpu.make_async_remote_copy(
            src_ref=source(h, block, 1 - core),
            dst_ref=theirs.at[h, block],
            send_sem=pair_send,
            recv_sem=here_sem.at[group_of[h, block]],
            device_id={"shard": partner},
            device_id_type=MESH,
        )

    def pair0(p, h, q):
        cols = pl.ds(q * width + p * size0, size0)
        return pltpu.make_async_remote_copy(
            src_ref=source(h, block_at(h, 2, 2), 1 - core).at[:, cols],
            dst_ref=theirs.at[h, block_at(h, 2, 2), :, cols],
            send_sem=pair_send,
            recv_sem=start_recv.at[p],
            device_id={"shard": partner},
            device_id_type=MESH,
        )

    def wait_bytes(ref, sem):
        pltpu.make_async_copy(ref, ref, sem).wait()

    def quarter(ref, h, block, q):
        return ref.at[h, block, :, pl.ds(q * width, width)]

    def send(link, src, dst, recv_sem, send_sem=link_send):
        pltpu.make_async_remote_copy(
            src_ref=src,
            dst_ref=dst,
            send_sem=send_sem,
            recv_sem=recv_sem,
            device_id={"shard": links[link]},
            device_id_type=MESH,
        ).start()

    def add_up(dst, terms):
        size = dst.shape[1]
        step = min(512, size)
        assert size % step == 0

        def one(i, _):
            cols = pl.ds(pl.multiple_of(i * step, step), step)
            if len(terms) == 2:
                dst[:, cols] = terms[0][:, cols] + terms[1][:, cols]
            else:
                total = terms[0][:, cols].astype(F32)
                for t in terms[1:]:
                    total = total + t[:, cols].astype(F32)
                dst[:, cols] = total.astype(BF16)
            return 0

        lax.fori_loop(0, size // step, one, 0)

    for h, block in groups[0] + groups[1]:
        load(h, block).start()
    with jax.named_scope("barrier"):
        @pl.when(core == 0)
        def _():
            pl.semaphore_wait(barrier, 1)

        @pl.when((core == 1) & jnp.logical_not(root))
        def _():
            pl.semaphore_wait(barrier, 1 + len(links))

        @pl.when(root)
        def _():
            pl.semaphore_wait(barrier, 1 + len(links) + n_section - 1)

        @pl.when(core == 1)
        def _():
            to_shards(heard.at[0], links)

    for p in range(PARTS0):
        for h, q in first4:
            pair0(p, h, q).start()
    small = [
        pltpu.make_async_copy(a, b, small_sem.at[k])
        for k, (a, b) in enumerate(((layer_hbm, layer), (valid_hbm, valid), (decay_hbm, decay)))
    ]
    io = [
        pltpu.make_async_copy(params, w_buf, io_sem.at[0]),
        pltpu.make_async_copy(m_first, f_buf, io_sem.at[1]),
        pltpu.make_async_copy(m_second, s_buf, io_sem.at[1]),
    ]
    for g in range(1, len(groups)):
        for h, block in groups[g]:
            pair(h, block).start()
        if g > 1:
            for h, block in groups[g]:
                load(h, block).start()
        if g == 4:
            for c in small + io:
                c.start()

    ready = {0}

    def need(h, block):
        g = group_of[h, block]
        if g not in ready:
            ready.add(g)
            count = 2 * len(groups[g])
            several = mine.at[0, pl.ds(0, count)] if count <= 16 else mine.at[:, pl.ds(0, count // 2)]
            wait_bytes(several, here_sem.at[g])

    signs = (1, 3)
    each = [(axis, d, 2 * axis + d) for axis in (0, 1) for d in (0, 1)]
    four, eight, sixteen = landed.at[0, pl.ds(0, 4)], landed.at[0, pl.ds(0, 8)], landed.at[pl.ds(0, 2), pl.ds(0, 8)]

    def own_terms(axis, block, q):
        need(axis, block)
        return [quarter(mine, axis, block, q), quarter(theirs, axis, block, q)]

    def far_first():
        wait_bytes(mine.at[0, pl.ds(0, 2)], here_sem.at[0])
        for p in range(PARTS0):
            wait_bytes(landed.at[0, 0, :, pl.ds(0, 4 * size0)], start_recv.at[p])
            if p == 0:

                @pl.when(core == 0)
                def _():
                    pl.semaphore_wait(near_in, 1)

            for axis, d, link in each:
                here = pl.ds(p * size0, size0)
                terms = [t.at[:, here] for t in own_terms(axis, block_at(axis, 2, 2), d)]
                add_up(terms[0], terms)
                send(link, terms[0], landed.at[link, FAR[0], :, here], far_recv.at[0])
        hear(0)

    def far(j):
        for axis, d, link in each:
            terms = own_terms(axis, block_at(axis, 2, ORDER[j]), d)
            add_up(terms[0], terms)
            send(link, terms[0], landed.at[link, FAR[j]], far_recv.at[j])

    def near_own(j):
        for axis, d, link in each:
            terms = own_terms(axis, block_at(axis, signs[d], ORDER[j]), 1 - d)
            add_up(terms[0], terms)
            send(link, terms[0], landed.at[link, NEAR_OWN[j]], near_recv.at[(0, 1, 1, 2)[j]])

    def near_sum(j):
        wait_bytes(four, far_recv.at[j])
        for axis, d, link in each:
            terms = own_terms(axis, block_at(axis, signs[d], ORDER[j]), d)
            add_up(terms[0], terms + [landed.at[link, FAR[j]]])
            send(link, terms[0], landed.at[link, NEAR_SUM[j]], near_recv.at[(0, 1, 1, 2)[j]])

    def first_axis(axis, j):
        block = block_at(axis, 0, ORDER[j])
        a, b = 2 * axis, 2 * axis + 1
        return [
            own_terms(axis, block, q)
            + [landed.at[(a, b)[q], NEAR_SUM[j]], landed.at[(b, a)[q], NEAR_OWN[j]]]
            for q in (0, 1)
        ]

    def settle(j):
        if j != 1:
            wait_bytes(eight if j == 0 else sixteen, near_recv.at[min(j, 1)])
        for axis in (0, 1):
            for terms in first_axis(axis, j):
                add_up(terms[0], terms)

    def far2():
        settle(0)
        for axis, d, _ in each:
            link = 2 * (1 - axis) + d
            send(link, quarter(mine, axis, block_at(axis, 0, 2), d), landed.at[link, FAR2], far2_recv)

    def own2():
        settle(2)
        settle(1)
        for axis, d, _ in each:
            link = 2 * (1 - axis) + d
            src = quarter(mine, axis, block_at(axis, 0, signs[d]), 1 - d)
            send(link, src, landed.at[link, OWN2], own2_recv, own2_send)

    def sum2():
        wait_bytes(four, far2_recv)

        for p, (start, size) in enumerate(parts):
            if p == 0:
                @pl.when(core == 1)
                def _():
                    pl.semaphore_wait(go_on, 1)

            for axis, d, _ in each:
                link = 2 * (1 - axis) + d
                at = pl.ds(start, size)
                dst = quarter(mine, axis, block_at(axis, 0, signs[d]), d).at[:, at]
                add_up(dst, [dst, landed.at[link, FAR2].at[:, at]])
                send(link, dst, late.at[link, :, at], sum2_recv.at[p], sum2_send)

    with jax.named_scope("far0"):
        far_first()
    for j in range(1, 4):
        with jax.named_scope(f"far{j}"):
            far(j)
        hear(j)
    for j in range(3):
        with jax.named_scope(f"own{j}"):
            near_own(j)
        with jax.named_scope(f"sum{j}"):
            near_sum(j)
        if j == 1:
            hear_roots()
    near_own(3)

    @pl.when(jnp.logical_not(root))
    def _():
        pl.semaphore_wait(all_in, 1)


    for c in small + io[:1]:
        c.wait()
    wait_bytes(theirs.at[0, pl.ds(0, 8)], io_sem.at[1])
    row_block = lax.broadcasted_iota(jnp.int32, (rows, 128), 0) // 8
    blocks = rows // 8

    def per_row(values):
        out = jnp.full((rows, 128), values[0])
        for b in range(1, blocks):
            out = jnp.where(row_block == b, values[b], out)
        return out

    layers = [layer[0, b] for b in range(blocks)]
    lives = [valid[0, b] for b in range(blocks)]
    row_decay = per_row([decay[l] for l in layers])
    row_live = per_row(lives) > 0

    row_layer = per_row(layers)
    row_lane = lax.broadcasted_iota(jnp.int32, (rows, 128), 1)
    own_lane = (row_lane == row_layer) & row_live
    own_lane_w = (row_lane == row_layer + 8) & row_live
    out_mask[...] = jnp.where(own_lane, 1.0, 0.0)

    def by_layer(total, lanes):
        in_row = jnp.sum(total, axis=1, keepdims=True)
        return jnp.sum(jnp.where(lanes, in_row, 0.0), axis=0, keepdims=True)

    piece = 512

    def weights_sq(i, acc):
        for k in range(piece // 128):
            v = w_buf[0, :, pl.ds(pl.multiple_of(i * piece + k * 128, 128), 128)].astype(F32)
            acc = acc + v * v
        return acc

    w_sum = by_layer(lax.fori_loop(0, columns // piece, weights_sq, jnp.zeros((rows, 128), F32)), own_lane_w)

    with jax.named_scope("far2"):
        far2()
    with jax.named_scope("near_sum3"):
        near_sum(3)
    with jax.named_scope("own2"):
        own2()
    with jax.named_scope("sum2"):
        sum2()

    with jax.named_scope("own2_sent"):
        wait_bytes(four, own2_send)

        @pl.when(core == 0)
        def _():
            to_shards(go_on, (partner,))

    with jax.named_scope("early"):
        wait_bytes(eight, near_recv.at[2])
        for axis in (0, 1):
            both = first_axis(axis, 3)
            if axis == 0:
                wait_bytes(four, own2_recv)
            for q in (0, 1):
                terms = both[q] + [landed.at[2 * (1 - axis) + 1 - q, OWN2]]
                base = (2 * axis + q) * width

                def before(i, _, terms=terms, base=base):
                    at = pl.multiple_of(i * min(512, width), min(512, width))
                    here = pl.ds(at, min(512, width))
                    g = terms[0][:, here].astype(F32)
                    for t in terms[1:]:
                        g = g + t[:, here].astype(F32)
                    upd[0, :, pl.ds(base + at, min(512, width))] = g
                    return 0

                lax.fori_loop(0, width // min(512, width), before, 0)

    acc = jnp.zeros((rows, 128), F32)
    for p, (start, part) in enumerate(parts):
        with jax.named_scope(f"late{p}"):
            wait_bytes(late.at[:, :, pl.ds(start, part)], sum2_recv.at[p])
        for axis in (0, 1):
            for q in (0, 1):
                came = late.at[2 * (1 - axis) + q, :, pl.ds(start, part)]
                base = (2 * axis + q) * width + start
                step = min(512, part)
                assert part % step == 0

                def one(i, acc, came=came, base=base, step=step):
                    for k in range(step // 128):
                        at = i * step + k * 128
                        cols = pl.ds(pl.multiple_of(base + at, 128), 128)
                        g = upd[0, :, cols] + came[:, pl.ds(pl.multiple_of(at, 128), 128)].astype(F32)
                        old_f, old_s = f_buf[0, :, cols], s_buf[0, :, cols]
                        w = w_buf[0, :, cols].astype(F32)
                        first = 0.9 * old_f + 0.1 * g
                        second = 0.99 * old_s + 0.01 * g * g
                        u = (first * (1.0 / bias_first)) / (
                            jnp.sqrt(second * (1.0 / bias_second)) + 1e-06
                        ) + row_decay * w
                        upd[0, :, cols] = u
                        f_buf[0, :, cols] = jnp.where(row_live, first, old_f)
                        s_buf[0, :, cols] = jnp.where(row_live, second, old_s)
                        acc = acc + u * u
                    return acc

                acc = lax.fori_loop(0, part // step, one, acc)

    vec = by_layer(acc, own_lane) + w_sum
    sums[0] = vec
    got[me] = vec

    def tell(to_section, to_shard):
        pltpu.make_async_remote_copy(
            src_ref=sums.at[0],
            dst_ref=got.at[me],
            send_sem=sum_send,
            recv_sem=sum_recv,
            device_id={"section": to_section, "shard": to_shard},
            device_id_type=MESH,
        ).start()

    far_from = (0, 1, 2, 1)
    away = sorted(
        ((ds, dy, dx, c) for ds in range(n_section) for dy in range(SIDE) for dx in range(SIDE) for c in (0, 1)),
        key=lambda a: -sum(far_from[k] for k in a[:3]) - a[3] / 2,
    )
    sections = [lax.rem(section + k, n_section) for k in range(n_section)]
    shards_at = {
        (dy, dx, c): chip_at(dy, dx) * 2 + (core if c == 0 else 1 - core)
        for dy in range(SIDE) for dx in range(SIDE) for c in (0, 1)
    }
    with jax.named_scope("tell"):
        for ds, dy, dx, c in away[:-1]:
            tell(sections[ds], shards_at[dy, dx, c])
    n_all = n_section * n_shard
    others = got.at[pl.ds(0, n_all - 1)]
    with jax.named_scope("everyone"):
        wait_bytes(others, sum_recv)

    with jax.named_scope("drain"):
        wait_bytes(theirs, pair_send)
        wait_bytes(landed.at[:, pl.ds(0, SLOTS - 1)], link_send)
        wait_bytes(late, sum2_send)
        wait_bytes(others, sum_send)


def finish(upd, first, second, weights, mask, got, out_params, out_first, out_second, out_ratios, stage, ratio, sem):
    columns = stage.shape[1]
    step = columns // 4
    copies = [
        pltpu.make_async_copy(first, out_first, sem.at[0]),
        pltpu.make_async_copy(second, out_second, sem.at[1]),
    ]
    for c in copies:
        c.start()
    several = [got[k] for k in range(8)]
    for k in range(8, got.shape[0]):
        several[k % 8] = several[k % 8] + got[k]
    while len(several) > 1:
        several = [a + b for a, b in zip(several[::2], several[1::2])]
    wide = jnp.broadcast_to(several[0], (8, 128))
    lane = lax.broadcasted_iota(jnp.int32, (1, 128), 1)
    ratios = jnp.sqrt(pltpu.roll(wide, 120, 1) / (wide + 1.0))[0:1]
    ratios = jnp.where(lane < ratio.shape[1], ratios, 0.0)
    ratio[...] = ratios[:, : ratio.shape[1]]
    c = pltpu.make_async_copy(ratio, out_ratios, sem.at[6])
    c.start()
    copies.append(c)
    row_ratio = jnp.sum(jnp.where(mask[...] > 0.5, ratios, 0.0), axis=1, keepdims=True)
    row_scale = jnp.broadcast_to(0.1 * row_ratio, mask.shape)
    for n in range(4):
      with jax.named_scope(f"fin{n}"):

        def one(i, _, n=n):
            for k in range(4):
                cols = pl.ds(pl.multiple_of(n * step + i * 512 + k * 128, 128), 128)
                w = weights[0, :, cols].astype(F32)
                stage[:, cols] = (w - row_scale * upd[0, :, cols]).astype(BF16)
            return 0

        lax.fori_loop(0, step // 512, one, 0)
        cols = pl.ds(n * step, step)
        c = pltpu.make_async_copy(stage.at[:, cols], out_params.at[0, :, cols], sem.at[2 + n])
        c.start()
        copies.append(c)
    with jax.named_scope("finw"):
      for c in copies:
        c.wait()


PARTS = (4, 4, 4, 2, 2)
PARTS0 = 4
ROUNDS = 4


def shards(grad_parts, params, moment_first, moment_second, block_layer, block_valid, decay):
    rows, columns = params.shape[1:]
    n_section, n_shard = lax.axis_size("section"), lax.axis_size("shard")
    width = columns // 4
    chips = SIDE * SIDE
    hbm, vmem = pl.BlockSpec(memory_space=pltpu.HBM), pl.BlockSpec(memory_space=pltpu.VMEM)
    dma = pltpu.SemaphoreType.DMA
    groups = 7
    upd, first, second, weights, mask, got = pl.pallas_call(
        functools.partial(kernel, n_section, n_shard),
        out_shape=(
            pltpu.VMEM(moment_first.shape, F32),
            pltpu.VMEM(moment_first.shape, F32),
            pltpu.VMEM(moment_first.shape, F32),
            pltpu.VMEM(params.shape, BF16),
            pltpu.VMEM((rows, 128), F32),
            pltpu.VMEM((n_section * n_shard, 1, 128), F32),
        ),
        in_specs=[hbm] * 7,
        out_specs=(vmem,) * 6,
        scratch_shapes=[
            pltpu.VMEM((2, chips, rows, 2 * width), BF16),
            pltpu.VMEM((2, chips, rows, 2 * width), BF16),
            pltpu.VMEM((4, SLOTS, rows, width), BF16),
            pltpu.VMEM((4, rows, width), BF16),
            pltpu.SMEM(block_layer.shape, jnp.int32),
            pltpu.SMEM(block_valid.shape, jnp.int32),
            pltpu.SMEM(decay.shape, F32),
            pltpu.VMEM((1, 1, 128), F32),
            dma((groups,)),
            dma,
            dma,
            dma((4,)),
            dma((3,)),
            dma,
            dma,
            dma,
            dma((len(PARTS),)),
            dma,
            dma((PARTS0,)),
            pltpu.SemaphoreType.REGULAR((ROUNDS,)),
            pltpu.SemaphoreType.REGULAR,
            pltpu.SemaphoreType.REGULAR,
            pltpu.SemaphoreType.REGULAR,
            pltpu.SemaphoreType.REGULAR,
            dma((3,)),
            dma((2,)),
            dma,
            dma,
        ],
        compiler_params=pltpu.CompilerParams(
            collective_id=0, has_side_effects=True, vmem_limit_bytes=48 * 2**20
        ),
        name="lamb_step",
    )(*(
        pltpu.with_memory_space_constraint(a, pltpu.HBM)
        for a in (grad_parts, params, moment_first, moment_second, block_layer, block_valid, decay)
    ))
    new_params, new_first, new_second, ratios = pl.pallas_call(
        finish,
        out_shape=(
            jax.ShapeDtypeStruct(params.shape, params.dtype),
            jax.ShapeDtypeStruct(moment_first.shape, F32),
            jax.ShapeDtypeStruct(moment_second.shape, F32),
            jax.ShapeDtypeStruct((1, decay.shape[0]), F32),
        ),
        in_specs=[vmem] * 6,
        out_specs=(hbm,) * 4,
        scratch_shapes=[pltpu.VMEM((rows, columns), BF16), pltpu.VMEM((1, decay.shape[0]), F32), dma((7,))],
        compiler_params=pltpu.CompilerParams(vmem_limit_bytes=8 * 2**20),
        name="finish",
    )(upd, first, second, weights, mask, got)
    return new_params, new_first, new_second, ratios[0]


def solution(mesh):
    placed = (
        P("section", "shard", None, None),
        P("section", "shard", None),
        P("section", "shard", None),
        P("section", "shard", None),
        P("section", "shard"),
        P("section", "shard"),
        P(),
    )
    return jax.shard_map(
        shards,
        mesh=mesh,
        in_specs=placed,
        out_specs=(
            P("section", "shard", None),
            P("section", "shard", None),
            P("section", "shard", None),
            P(),
        ),
        check_vma=False,
    )
```

```python
import functools

import jax
import jax.numpy as jnp
from jax import lax
from jax.experimental import pallas as pl
from jax.experimental.pallas import tpu as pltpu
from jax.sharding import PartitionSpec as P

bias_first = 1.0 - 0.9**10
bias_second = 1.0 - 0.99**10

MESH = pl.DeviceIdType.MESH
F32, BF16 = jnp.float32, jnp.bfloat16
SIDE = 4
ORDER = (2, 1, 3, 0)
FAR, NEAR_OWN, NEAR_SUM = (0, 1, 2, 3), (4, 6, 8, 10), (5, 7, 9, 11)
FAR2, OWN2 = 12, 13
SLOTS = 14


def block_at(axis, main, other):
    return other * SIDE + main if axis == 0 else main * SIDE + other


def kernel(
    n_section, n_shard,
    grads, params, m_first, m_second, layer_hbm, valid_hbm, decay_hbm,
    upd, f_buf, s_buf, w_buf, out_mask, got,
    mine, theirs, landed, late, layer, valid, decay, sums,
    here_sem, pair_send, link_send, far_recv, near_recv, far2_recv, own2_recv, own2_send, sum2_recv, sum2_send,
    start_recv, heard, near_in, roots_in, all_in, go_on, small_sem, io_sem, sum_send, sum_recv,
):
    rows = w_buf.shape[1]
    columns = w_buf.shape[2]
    width = landed.shape[3]
    parts = [(sum(PARTS[:p]) * (width // 16), PARTS[p] * (width // 16)) for p in range(len(PARTS))]
    section, shard = lax.axis_index("section"), lax.axis_index("shard")
    core, x, y = lax.rem(shard, 2), lax.rem(lax.div(shard, 2), SIDE), lax.div(shard, 2 * SIDE)
    me = section * n_shard + shard
    partner = shard + 1 - 2 * core

    def chip_at(dy, dx):
        return lax.rem(y + dy, SIDE) * SIDE + lax.rem(x + dx, SIDE)

    links = tuple(chip_at(dy, dx) * 2 + core for dy, dx in ((0, 1), (0, 3), (1, 0), (3, 0)))

    root = (core == 1) & (x == 0) & (y == 0)

    def to_shards(sem, peers):
        for peer in peers:
            pl.semaphore_signal(sem, inc=1, device_id={"shard": peer}, device_id_type=MESH)

    def to_roots(sem):
        for k in range(1, n_section):
            pl.semaphore_signal(
                sem, inc=1, device_id={"section": lax.rem(section + k, n_section)}, device_id_type=MESH
            )

    barrier = pltpu.get_barrier_semaphore()
    to_shards(barrier, (partner,))

    @pl.when(core == 1)
    def _():
        to_shards(barrier, links)

    @pl.when(root)
    def _():
        to_roots(barrier)

    def hear(k):
        @pl.when(core == 1)
        def _():
            pl.semaphore_wait(heard.at[k], len(links))
            if k + 1 < ROUNDS:
                to_shards(heard.at[k + 1], links)
            if k == 0:
                to_shards(near_in, (partner,))

        if k + 1 == ROUNDS:

            @pl.when(root)
            def _():
                to_roots(roots_in)

    def hear_roots():
        @pl.when(root)
        def _():
            pl.semaphore_wait(roots_in, n_section - 1)
            to_shards(all_in, [k for k in range(n_shard) if k != 1])

    groups = []
    for j in ORDER:
        groups.append([(h, block_at(h, 2, j)) for h in (0, 1)])
    for j in ORDER:
        groups.append([(h, block_at(h, main, j)) for main in (1, 3, 0) for h in (0, 1)])
    group_of = {b: g for g, blocks in enumerate(groups) for b in blocks}

    size0 = width // PARTS0
    first4 = [(h, q) for h in (0, 1) for q in (0, 1)]

    def source(h, block, which):
        chip = chip_at(block // SIDE, block % SIDE)
        at = pl.multiple_of(chip * (2 * rows) + which * rows, rows)
        return grads.at[0, 0, pl.ds(at, rows), pl.ds(h * 2 * width, 2 * width)]

    def load(h, block):
        return pltpu.make_async_copy(
            source(h, block, core), mine.at[h, block], here_sem.at[group_of[h, block]]
        )

    def load(h, block):
        return pltpu.make_async_copy(
            source(h, block, core), mine.at[h, block], here_sem.at[group_of[h, block]]
        )

    def fetch_ahead(p, h, q):
        cols = pl.ds(q * width + p * size0, size0)
        return pltpu.make_async_copy(
            source(h, block_at(h, 2, 2), 1 - core).at[:, cols], ahead.at[h, :, cols], ahead_sem.at[p]
        )

    def pair(h, block):
        return pltpu.make_async_remote_copy(
            src_ref=source(h, block, 1 - core),
            dst_ref=theirs.at[h, block],
            send_sem=pair_send,
            recv_sem=here_sem.at[group_of[h, block]],
            device_id={"shard": partner},
            device_id_type=MESH,
        )

    def pair0(p, h, q):
        cols = pl.ds(q * width + p * size0, size0)
        return pltpu.make_async_remote_copy(
            src_ref=source(h, block_at(h, 2, 2), 1 - core).at[:, cols],
            dst_ref=theirs.at[h, block_at(h, 2, 2), :, cols],
            send_sem=pair_send,
            recv_sem=start_recv.at[p],
            device_id={"shard": partner},
            device_id_type=MESH,
        )

    def wait_bytes(ref, sem):
        pltpu.make_async_copy(ref, ref, sem).wait()

    def quarter(ref, h, block, q):
        return ref.at[h, block, :, pl.ds(q * width, width)]

    def send(link, src, dst, recv_sem, send_sem=link_send):
        pltpu.make_async_remote_copy(
            src_ref=src,
            dst_ref=dst,
            send_sem=send_sem,
            recv_sem=recv_sem,
            device_id={"shard": links[link]},
            device_id_type=MESH,
        ).start()

    def add_up(dst, terms):
        size = dst.shape[1]
        step = min(512, size)
        assert size % step == 0

        def one(i, _):
            cols = pl.ds(pl.multiple_of(i * step, step), step)
            if len(terms) == 2:
                dst[:, cols] = terms[0][:, cols] + terms[1][:, cols]
            else:
                total = terms[0][:, cols].astype(F32)
                for t in terms[1:]:
                    total = total + t[:, cols].astype(F32)
                dst[:, cols] = total.astype(BF16)
            return 0

        lax.fori_loop(0, size // step, one, 0)

    for h, block in groups[0]:
        load(h, block).start()
    with jax.named_scope("barrier"):
        @pl.when(core == 0)
        def _():
            pl.semaphore_wait(barrier, 1)

        @pl.when((core == 1) & jnp.logical_not(root))
        def _():
            pl.semaphore_wait(barrier, 1 + len(links))

        @pl.when(root)
        def _():
            pl.semaphore_wait(barrier, 1 + len(links) + n_section - 1)

        @pl.when(core == 1)
        def _():
            to_shards(heard.at[0], links)

    for p in range(PARTS0):
        for h, q in first4:
            pair0(p, h, q).start()
    small = [
        pltpu.make_async_copy(a, b, small_sem.at[k])
        for k, (a, b) in enumerate(((layer_hbm, layer), (valid_hbm, valid), (decay_hbm, decay)))
    ]
    io = [
        pltpu.make_async_copy(params, w_buf, io_sem.at[0]),
        pltpu.make_async_copy(m_first, f_buf, io_sem.at[1]),
        pltpu.make_async_copy(m_second, s_buf, io_sem.at[1]),
    ]
    for g in range(1, len(groups)):
        for h, block in groups[g]:
            pair(h, block).start()
        for h, block in groups[g]:
            load(h, block).start()
        if g == 4:
            for c in small + io:
                c.start()

    ready = {0}

    def need(h, block):
        g = group_of[h, block]
        if g not in ready:
            ready.add(g)
            wait_bytes(mine.at[0, pl.ds(0, 2 * len(groups[g]))], here_sem.at[g])

    signs = (1, 3)
    each = [(axis, d, 2 * axis + d) for axis in (0, 1) for d in (0, 1)]
    four, eight = landed.at[0, pl.ds(0, 4)], landed.at[0, pl.ds(0, 8)]

    def own_terms(axis, block, q):
        need(axis, block)
        return [quarter(mine, axis, block, q), quarter(theirs, axis, block, q)]

    def far_first():
        wait_bytes(mine.at[0, pl.ds(0, 2)], here_sem.at[0])
        for p in range(PARTS0):
            wait_bytes(landed.at[0, 0, :, pl.ds(0, 4 * size0)], start_recv.at[p])
            if p == 0:

                @pl.when(core == 0)
                def _():
                    pl.semaphore_wait(near_in, 1)

            for axis, d, link in each:
                here = pl.ds(p * size0, size0)
                terms = [t.at[:, here] for t in own_terms(axis, block_at(axis, 2, 2), d)]
                add_up(terms[0], terms)
                send(link, terms[0], landed.at[link, FAR[0], :, here], far_recv.at[0])
        hear(0)

    def far(j):
        for axis, d, link in each:
            terms = own_terms(axis, block_at(axis, 2, ORDER[j]), d)
            add_up(terms[0], terms)
            send(link, terms[0], landed.at[link, FAR[j]], far_recv.at[j])

    def near_own(j):
        for axis, d, link in each:
            terms = own_terms(axis, block_at(axis, signs[d], ORDER[j]), 1 - d)
            add_up(terms[0], terms)
            send(link, terms[0], landed.at[link, NEAR_OWN[j]], near_recv.at[j])

    def near_sum(j):
        wait_bytes(four, far_recv.at[j])
        for axis, d, link in each:
            terms = own_terms(axis, block_at(axis, signs[d], ORDER[j]), d)
            add_up(terms[0], terms + [landed.at[link, FAR[j]]])
            send(link, terms[0], landed.at[link, NEAR_SUM[j]], near_recv.at[j])

    def first_axis(axis, j):
        block = block_at(axis, 0, ORDER[j])
        a, b = 2 * axis, 2 * axis + 1
        return [
            own_terms(axis, block, q)
            + [landed.at[(a, b)[q], NEAR_SUM[j]], landed.at[(b, a)[q], NEAR_OWN[j]]]
            for q in (0, 1)
        ]

    def settle(j):
        wait_bytes(eight, near_recv.at[j])
        for axis in (0, 1):
            for terms in first_axis(axis, j):
                add_up(terms[0], terms)

    def far2():
        settle(0)
        for axis, d, _ in each:
            link = 2 * (1 - axis) + d
            send(link, quarter(mine, axis, block_at(axis, 0, 2), d), landed.at[link, FAR2], far2_recv)

    def own2():
        settle(1)
        settle(2)
        for axis, d, _ in each:
            link = 2 * (1 - axis) + d
            src = quarter(mine, axis, block_at(axis, 0, signs[d]), 1 - d)
            send(link, src, landed.at[link, OWN2], own2_recv, own2_send)

    def sum2():
        wait_bytes(four, far2_recv)

        for p, (start, size) in enumerate(parts):
            if p == 0:
                @pl.when(core == 1)
                def _():
                    pl.semaphore_wait(go_on, 1)

            for axis, d, _ in each:
                link = 2 * (1 - axis) + d
                at = pl.ds(start, size)
                dst = quarter(mine, axis, block_at(axis, 0, signs[d]), d).at[:, at]
                add_up(dst, [dst, landed.at[link, FAR2].at[:, at]])
                send(link, dst, late.at[link, :, at], sum2_recv.at[p], sum2_send)

    with jax.named_scope("far0"):
        far_first()
    for j in range(1, 4):
        with jax.named_scope(f"far{j}"):
            far(j)
        hear(j)
    for j in range(3):
        with jax.named_scope(f"own{j}"):
            near_own(j)
        with jax.named_scope(f"sum{j}"):
            near_sum(j)
        if j == 1:
            hear_roots()
    near_own(3)

    @pl.when(jnp.logical_not(root))
    def _():
        pl.semaphore_wait(all_in, 1)


    for c in small + io[:1]:
        c.wait()
    wait_bytes(theirs.at[0, pl.ds(0, 8)], io_sem.at[1])
    row_block = lax.broadcasted_iota(jnp.int32, (rows, 128), 0) // 8
    blocks = rows // 8

    def per_row(values):
        out = jnp.full((rows, 128), values[0])
        for b in range(1, blocks):
            out = jnp.where(row_block == b, values[b], out)
        return out

    layers = [layer[0, b] for b in range(blocks)]
    lives = [valid[0, b] for b in range(blocks)]
    row_decay = per_row([decay[l] for l in layers])
    row_live = per_row(lives) > 0

    row_layer = per_row(layers)
    row_lane = lax.broadcasted_iota(jnp.int32, (rows, 128), 1)
    own_lane = (row_lane == row_layer) & row_live
    own_lane_w = (row_lane == row_layer + 8) & row_live
    out_mask[...] = jnp.where(own_lane, 1.0, 0.0)

    def by_layer(total, lanes):
        in_row = jnp.sum(total, axis=1, keepdims=True)
        return jnp.sum(jnp.where(lanes, in_row, 0.0), axis=0, keepdims=True)

    piece = 512

    def weights_sq(i, acc):
        for k in range(piece // 128):
            v = w_buf[0, :, pl.ds(pl.multiple_of(i * piece + k * 128, 128), 128)].astype(F32)
            acc = acc + v * v
        return acc

    w_sum = by_layer(lax.fori_loop(0, columns // piece, weights_sq, jnp.zeros((rows, 128), F32)), own_lane_w)

    with jax.named_scope("far2"):
        far2()
    with jax.named_scope("near_sum3"):
        near_sum(3)
    with jax.named_scope("own2"):
        own2()
    with jax.named_scope("sum2"):
        sum2()

    with jax.named_scope("own2_sent"):
        wait_bytes(four, own2_send)

        @pl.when(core == 0)
        def _():
            to_shards(go_on, (partner,))

    with jax.named_scope("early"):
        wait_bytes(eight, near_recv.at[3])
        for axis in (0, 1):
            both = first_axis(axis, 3)
            if axis == 0:
                wait_bytes(four, own2_recv)
            for q in (0, 1):
                terms = both[q] + [landed.at[2 * (1 - axis) + 1 - q, OWN2]]
                base = (2 * axis + q) * width

                def before(i, _, terms=terms, base=base):
                    at = pl.multiple_of(i * min(512, width), min(512, width))
                    here = pl.ds(at, min(512, width))
                    g = terms[0][:, here].astype(F32)
                    for t in terms[1:]:
                        g = g + t[:, here].astype(F32)
                    upd[0, :, pl.ds(base + at, min(512, width))] = g
                    return 0

                lax.fori_loop(0, width // min(512, width), before, 0)

    acc = jnp.zeros((rows, 128), F32)
    for p, (start, part) in enumerate(parts):
        with jax.named_scope(f"late{p}"):
            wait_bytes(late.at[:, :, pl.ds(start, part)], sum2_recv.at[p])
        for axis in (0, 1):
            for q in (0, 1):
                came = late.at[2 * (1 - axis) + q, :, pl.ds(start, part)]
                base = (2 * axis + q) * width + start
                step = min(512, part)
                assert part % step == 0

                def one(i, acc, came=came, base=base, step=step):
                    for k in range(step // 128):
                        at = i * step + k * 128
                        cols = pl.ds(pl.multiple_of(base + at, 128), 128)
                        g = upd[0, :, cols] + came[:, pl.ds(pl.multiple_of(at, 128), 128)].astype(F32)
                        old_f, old_s = f_buf[0, :, cols], s_buf[0, :, cols]
                        w = w_buf[0, :, cols].astype(F32)
                        first = 0.9 * old_f + 0.1 * g
                        second = 0.99 * old_s + 0.01 * g * g
                        u = (first * (1.0 / bias_first)) / (
                            jnp.sqrt(second * (1.0 / bias_second)) + 1e-06
                        ) + row_decay * w
                        upd[0, :, cols] = u
                        f_buf[0, :, cols] = jnp.where(row_live, first, old_f)
                        s_buf[0, :, cols] = jnp.where(row_live, second, old_s)
                        acc = acc + u * u
                    return acc

                acc = lax.fori_loop(0, part // step, one, acc)

    vec = by_layer(acc, own_lane) + w_sum
    sums[0] = vec
    got[me] = vec

    def tell(to_section, to_shard):
        pltpu.make_async_remote_copy(
            src_ref=sums.at[0],
            dst_ref=got.at[me],
            send_sem=sum_send,
            recv_sem=sum_recv,
            device_id={"section": to_section, "shard": to_shard},
            device_id_type=MESH,
        ).start()

    far_from = (0, 1, 2, 1)
    away = sorted(
        ((ds, dy, dx, c) for ds in range(n_section) for dy in range(SIDE) for dx in range(SIDE) for c in (0, 1)),
        key=lambda a: -sum(far_from[k] for k in a[:3]) - a[3] / 2,
    )
    sections = [lax.rem(section + k, n_section) for k in range(n_section)]
    shards_at = {
        (dy, dx, c): chip_at(dy, dx) * 2 + (core if c == 0 else 1 - core)
        for dy in range(SIDE) for dx in range(SIDE) for c in (0, 1)
    }
    with jax.named_scope("tell"):
        for ds, dy, dx, c in away[:-1]:
            tell(sections[ds], shards_at[dy, dx, c])
    n_all = n_section * n_shard
    others = got.at[pl.ds(0, n_all - 1)]
    with jax.named_scope("everyone"):
        wait_bytes(others, sum_recv)

    with jax.named_scope("drain"):
        wait_bytes(theirs, pair_send)
        wait_bytes(landed.at[:, pl.ds(0, SLOTS - 1)], link_send)
        wait_bytes(late, sum2_send)
        wait_bytes(others, sum_send)


def finish(upd, first, second, weights, mask, got, out_params, out_first, out_second, out_ratios, stage, ratio, sem):
    columns = stage.shape[1]
    step = columns // 4
    copies = [
        pltpu.make_async_copy(first, out_first, sem.at[0]),
        pltpu.make_async_copy(second, out_second, sem.at[1]),
    ]
    for c in copies:
        c.start()
    several = [got[k] for k in range(8)]
    for k in range(8, got.shape[0]):
        several[k % 8] = several[k % 8] + got[k]
    while len(several) > 1:
        several = [a + b for a, b in zip(several[::2], several[1::2])]
    wide = jnp.broadcast_to(several[0], (8, 128))
    lane = lax.broadcasted_iota(jnp.int32, (1, 128), 1)
    ratios = jnp.sqrt(pltpu.roll(wide, 120, 1) / (wide + 1.0))[0:1]
    ratios = jnp.where(lane < ratio.shape[1], ratios, 0.0)
    ratio[...] = ratios[:, : ratio.shape[1]]
    c = pltpu.make_async_copy(ratio, out_ratios, sem.at[3])
    c.start()
    copies.append(c)
    row_ratio = jnp.sum(jnp.where(mask[...] > 0.5, ratios, 0.0), axis=1, keepdims=True)
    row_scale = jnp.broadcast_to(0.1 * row_ratio, mask.shape)
    for n in range(4):
      with jax.named_scope(f"fin{n}"):

        def one(i, _, n=n):
            for k in range(4):
                cols = pl.ds(pl.multiple_of(n * step + i * 512 + k * 128, 128), 128)
                w = weights[0, :, cols].astype(F32)
                stage[:, cols] = (w - row_scale * upd[0, :, cols]).astype(BF16)
            return 0

        lax.fori_loop(0, step // 512, one, 0)
        cols = pl.ds(n * step, step)
        pltpu.make_async_copy(stage.at[:, cols], out_params.at[0, :, cols], sem.at[2]).start()
    with jax.named_scope("finw"):
      for c in copies:
        c.wait()
      pltpu.make_async_copy(stage, out_params.at[0], sem.at[2]).wait()


PARTS = (4, 4, 4, 2, 2)
PARTS0 = 4
ROUNDS = 4


def shards(grad_parts, params, moment_first, moment_second, block_layer, block_valid, decay):
    rows, columns = params.shape[1:]
    n_section, n_shard = lax.axis_size("section"), lax.axis_size("shard")
    width = columns // 4
    chips = SIDE * SIDE
    hbm, vmem = pl.BlockSpec(memory_space=pltpu.HBM), pl.BlockSpec(memory_space=pltpu.VMEM)
    dma = pltpu.SemaphoreType.DMA
    groups = 8
    upd, first, second, weights, mask, got = pl.pallas_call(
        functools.partial(kernel, n_section, n_shard),
        out_shape=(
            pltpu.VMEM(moment_first.shape, F32),
            pltpu.VMEM(moment_first.shape, F32),
            pltpu.VMEM(moment_first.shape, F32),
            pltpu.VMEM(params.shape, BF16),
            pltpu.VMEM((rows, 128), F32),
            pltpu.VMEM((n_section * n_shard, 1, 128), F32),
        ),
        in_specs=[hbm] * 7,
        out_specs=(vmem,) * 6,
        scratch_shapes=[
            pltpu.VMEM((2, chips, rows, 2 * width), BF16),
            pltpu.VMEM((2, chips, rows, 2 * width), BF16),
            pltpu.VMEM((4, SLOTS, rows, width), BF16),
            pltpu.VMEM((4, rows, width), BF16),
            pltpu.SMEM(block_layer.shape, jnp.int32),
            pltpu.SMEM(block_valid.shape, jnp.int32),
            pltpu.SMEM(decay.shape, F32),
            pltpu.VMEM((1, 1, 128), F32),
            dma((groups,)),
            dma,
            dma,
            dma((4,)),
            dma((4,)),
            dma,
            dma,
            dma,
            dma((len(PARTS),)),
            dma,
            dma((PARTS0,)),
            pltpu.SemaphoreType.REGULAR((ROUNDS,)),
            pltpu.SemaphoreType.REGULAR,
            pltpu.SemaphoreType.REGULAR,
            pltpu.SemaphoreType.REGULAR,
            pltpu.SemaphoreType.REGULAR,
            dma((3,)),
            dma((2,)),
            dma,
            dma,
        ],
        compiler_params=pltpu.CompilerParams(
            collective_id=0, has_side_effects=True, vmem_limit_bytes=48 * 2**20
        ),
        name="lamb_step",
    )(*(
        pltpu.with_memory_space_constraint(a, pltpu.HBM)
        for a in (grad_parts, params, moment_first, moment_second, block_layer, block_valid, decay)
    ))
    new_params, new_first, new_second, ratios = pl.pallas_call(
        finish,
        out_shape=(
            jax.ShapeDtypeStruct(params.shape, params.dtype),
            jax.ShapeDtypeStruct(moment_first.shape, F32),
            jax.ShapeDtypeStruct(moment_second.shape, F32),
            jax.ShapeDtypeStruct((1, decay.shape[0]), F32),
        ),
        in_specs=[vmem] * 6,
        out_specs=(hbm,) * 4,
        scratch_shapes=[pltpu.VMEM((rows, columns), BF16), pltpu.VMEM((1, decay.shape[0]), F32), dma((4,))],
        compiler_params=pltpu.CompilerParams(vmem_limit_bytes=8 * 2**20),
        name="finish",
    )(upd, first, second, weights, mask, got)
    return new_params, new_first, new_second, ratios[0]


def solution(mesh):
    placed = (
        P("section", "shard", None, None),
        P("section", "shard", None),
        P("section", "shard", None),
        P("section", "shard", None),
        P("section", "shard"),
        P("section", "shard"),
        P(),
    )
    return jax.shard_map(
        shards,
        mesh=mesh,
        in_specs=placed,
        out_specs=(
            P("section", "shard", None),
            P("section", "shard", None),
            P("section", "shard", None),
            P(),
        ),
        check_vma=False,
    )
```
